32 devices in a mesh: seq: 8 (over z, x), wsh: 4 (over y, core).
Axes of the slice: x: 2, y: 2, z: 4, core: 2. Of those that a mesh axis runs over, the one named last changes fastest.
Arguments:
- tokens_in: bfloat16 [4, 4096, 1024], P('wsh', 'seq'), may hold values from -6 to 6
- out_grad: bfloat16 [4, 4096, 1024], P('wsh', 'seq'), may hold values from -6 to 6
- deal_order: int32 [8], replicated, may hold values from 0 to 7, each once
- seq_lengths: int32 [4, 4], P('wsh'), may hold values from 1 to 2048, 4096 in all within a row
- weights: bfloat16 [1024, 17920], P('wsh'), may hold values from -0.1875 to 0.1875
- norm_gains: bfloat16 [2, 1024], P(None, 'wsh'), may hold values from 0.5 to 1.5
- conv_kernel: bfloat16 [3, 1024], P(None, 'wsh'), may hold values from -3 to 3
- vector_state: float32 [5, 1024], P(None, 'wsh'), may hold values from 0.2 to 5
- kron_stats: float32 [2, 1120, 128, 128], P(None, 'wsh', 'seq'), may hold values from -6 to 6
- kron_roots: float32 [2, 1120, 128, 128], P(None, 'wsh', 'seq'), as said below
Outputs:
- block_out: bfloat16 [4, 4096, 1024], P('wsh', 'seq')
- input_grad: bfloat16 [4, 4096, 1024], P('wsh', 'seq')
- weight_grad: float32 [1024, 17920], P('wsh')
- vector_grad: float32 [5, 1024], P(None, 'wsh')
- vector_state_new: float32 [5, 1024], P(None, 'wsh')
- vector_update: float32 [5, 1024], P(None, 'wsh')
- kron_stats_new: float32 [2, 1120, 128, 128], P(None, 'wsh', 'seq')
- weight_update: float32 [1120, 128, 128], P('wsh', 'seq')
The draws below stay inside these ranges and needn't reach their ends.
Inputs may be any that keep to these rules, and one draw needn't show every extreme that they name: `deal_order`: a permutation of 0 to 7. `seq_lengths`: each row sums to 4096; in every pack the longest sequence has exactly 2048 tokens. `kron_roots`: each block has a dominant diagonal between 0.5 and 2.
All inputs are finite; a program needn't handle non-finite values.
Results may differ from the reference program's by a relative error of at most 0.025.
Values may be sent and summed in bfloat16 or wider, within the bound.
A program may use at most 320 MiB of HBM per device.

```python
import math
import jax
import jax.numpy as jnp
import numpy as np
from jax import lax

D = 1024
FF = 4608
BLK = 128
TOK_DEV = 512
SEQS = 4
PACK = 4096
PACKS = 4
TOKENS = 16384
LONGEST = 2048
WCOLS = 17920
NBLK = 1120
N_SEQ = 8


def draw_kron_roots(key, part):
    key_diag = jax.random.fold_in(key, 11)
    key_off = jax.random.fold_in(key, 12)
    diag = jnp.exp(jax.random.uniform(key_diag, (2, NBLK, BLK, 1), jnp.float32, -0.69, 0.69))
    off = jax.random.normal(key_off, (2, NBLK, BLK, BLK), jnp.float32) * (0.45 / math.sqrt(BLK))
    rows_at = lax.broadcasted_iota(jnp.int32, (BLK, BLK), 0)
    cols_at = lax.broadcasted_iota(jnp.int32, (BLK, BLK), 1)
    same = (rows_at == cols_at)[None, None]
    return jnp.where(same, jnp.broadcast_to(diag, (2, NBLK, BLK, BLK)), off).astype(jnp.float32)


def block_scale(stream_key, shape, shards, least, largest):
    def one(dim, shards_of):
        draws = jax.random.uniform(jax.random.fold_in(jax.random.fold_in(stream_key, 6), dim), (shards_of,), jnp.float32, least / len(shards), largest / len(shards))
        return jnp.repeat(jnp.exp(draws), shape[dim] // shards_of).reshape((-1,) + (1,) * (len(shape) - dim - 1))

    level = one(*shards[0])
    for cut in shards[1:]:
        level = level * one(*cut)
    return level


def length_profile(count, total, most, skew):
    loads = [(1 << 20) // math.isqrt(grade ** skew) + 1 for grade in range(2, count + 1)]
    surplus, counts = total - most - (count - 1), [1] * (count - 1)
    while surplus > 0:
        free = [i for i in range(count - 1) if counts[i] < most]
        pool, left = sum([loads[i] for i in free]), surplus
        for i in free:
            addition = min(most - counts[i], max(1, left * loads[i] // pool), surplus)
            counts[i] = counts[i] + addition
            surplus = surplus - addition
    return np.array([most] + counts)


def ragged_sizes(own_key, amount, total, most, skew):
    if amount == 2:
        one = jax.random.randint(own_key, (), max(1, total - most), min(most, total - 1) + 1)
        return jnp.stack([one, total - one])
    tallies = jnp.asarray(length_profile(amount, total, most, skew), jnp.int32)
    twos = (amount - 1) // 2
    source_of, sink = tallies[1:1 + 2 * twos:2], tallies[2:2 + 2 * twos:2]
    margin = jnp.minimum(source_of - 1, most - sink)
    passed = jax.random.randint(jax.random.fold_in(own_key, 1), (twos,), 0, 1 << 20) % (margin + 1)
    tallies = tallies.at[1:1 + 2 * twos:2].set(source_of - passed).at[2:2 + 2 * twos:2].set(sink + passed)
    return tallies[jax.random.permutation(jax.random.fold_in(own_key, 2), amount)]


def bell_draw(rng, shape, scale, most, pieces=(), kind=jnp.bfloat16):
    gain = block_scale(rng, shape, pieces, -0.22, 0.18) if pieces else 1.0
    values = jax.random.normal(rng, shape, jnp.float32) * scale * gain
    return jnp.minimum(jnp.maximum(values, -most), most).astype(kind)


def setup_inputs(seed: int = 0) -> dict:
    streams_of = jax.random.split(jax.random.key(seed), 11)
    return {
        "tokens_in": bell_draw(streams_of[0], (PACKS, PACK, D), 1.0, 6.0, ((0, 4), (1, 8))),
        "out_grad": bell_draw(streams_of[1], (PACKS, PACK, D), 1.0, 6.0, ((0, 4), (1, 8))),
        "deal_order": jax.random.permutation(streams_of[2], N_SEQ).astype(jnp.int32),
        "seq_lengths": jax.vmap(lambda own: ragged_sizes(own, SEQS, TOK_DEV * N_SEQ, LONGEST, 2))(jax.random.split(streams_of[3], PACKS)).reshape((PACKS, SEQS)).astype(jnp.int32),
        "weights": bell_draw(streams_of[4], (D, WCOLS), D ** -0.5, 0.1875, ((0, 4),)),
        "norm_gains": jnp.clip(1.0 + 0.1 * jax.random.normal(streams_of[5], (2, D), jnp.float32), 0.5, 1.5).astype(jnp.bfloat16),
        "conv_kernel": bell_draw(streams_of[6], (3, D), 0.6, 3.0, ((1, 4),)),
        "vector_state": jnp.clip(jnp.exp(math.log(5.0) - 3.218876 * jax.random.uniform(streams_of[7], (5, D), jnp.float32) ** block_scale(streams_of[7], (5, D), ((1, 4),), -0.2, 0.2)), 0.2, 5.0),
        "kron_stats": bell_draw(streams_of[8], (2, NBLK, BLK, BLK), 1.0, 6.0, ((1, 4), (2, 8)), jnp.float32),
        "kron_roots": draw_kron_roots(jax.random.fold_in(streams_of[10], 71), 0),
    }


EPS = 1e-05
BETA = 0.5
BETA_VEC = 0.5
LEARN = 0.03
LEARN_VEC = 0.05
HIGH = lax.Precision.HIGHEST

@jax.custom_vjp
def low(v):
    return lax.optimization_barrier(v.astype(jnp.bfloat16)).astype(jnp.float32)

@jax.custom_vjp
def low_back(v):
    return v

def low_keep(v):
    return (low(v), None)

def low_pass(kept, grad):
    return (grad,)

def back_keep(v):
    return (v, None)

def back_low(kept, grad):
    return (low(grad),)
low.defvjp(low_keep, low_pass)
low_back.defvjp(back_keep, back_low)

def hi_dot(left, right):
    return jnp.dot(left, right, precision=HIGH, preferred_element_type=jnp.float32)

def seq_positions(lengths_row):
    lengths_row = lengths_row.astype(jnp.int32)
    starts = (jnp.cumsum(lengths_row) - lengths_row).astype(jnp.int32)
    rows_at = jnp.arange(PACK, dtype=jnp.int32)
    begin = lax.optimization_barrier(jnp.max(jnp.where(starts[None, :] <= rows_at[:, None], starts[None, :], 0), axis=1)).astype(jnp.int32)
    return rows_at - begin

def rms_scale(v):
    return lax.rsqrt(lax.optimization_barrier(jnp.mean(v * v, axis=1, keepdims=True)) + EPS)

def layer(wfull, gains, kernel, xs, pos):
    w_in = wfull[:, :3 * D]
    w_out = wfull[:, 3 * D:4 * D]
    w_gu = wfull[:, 4 * D:4 * D + 2 * FF]
    w_down = wfull[:, 4 * D + 2 * FF:]

    def step(prev, inputs):
        xb, pb = inputs
        count = xb.shape[0]
        scale_one = rms_scale(xb)
        xn = low(xb * scale_one * gains[0])
        proj = low_back(hi_dot(xn, w_in))
        b_part = proj[:, :D]
        c_part = proj[:, D:2 * D]
        x_part = proj[:, 2 * D:]
        bx = b_part * x_part
        ext = jnp.concatenate([prev, bx], axis=0)
        conv = jnp.zeros_like(bx)
        for k in range(3):
            mask = (pb >= 2 - k).astype(jnp.float32)[:, None]
            conv = conv + kernel[k] * mask * ext[k:k + count]
        yc = low(c_part * conv)
        mix = low_back(hi_dot(yc, w_out))
        hidden_sum = xb + mix
        scale_two = rms_scale(hidden_sum)
        hn = low(hidden_sum * scale_two * gains[1])
        gate_up = low_back(hi_dot(hn, w_gu))
        act = low(jax.nn.silu(gate_up[:, :FF]) * gate_up[:, FF:])
        ffn = lax.dot_general(act, w_down, (((1,), (1,)), ((), ())), precision=HIGH, preferred_element_type=jnp.float32)
        return (bx[count - 2:], hidden_sum + ffn)
    rows_block = min(4096, TOKENS)
    nblocks = TOKENS // rows_block
    carry0 = jnp.zeros((2, D), jnp.float32)
    _, outs = lax.scan(jax.checkpoint(step), carry0, (xs.reshape(nblocks, rows_block, D), pos.reshape(nblocks, rows_block)))
    return outs.reshape(TOKENS, D)

def reference(tokens_in, out_grad, deal_order, seq_lengths, weights, norm_gains, conv_kernel, vector_state, kron_stats, kron_roots):
    unit_rows = TOK_DEV // N_SEQ
    prow = jnp.arange(PACK, dtype=jnp.int32)
    unit_of = prow // unit_rows
    within = prow % unit_rows
    slot = unit_of // N_SEQ
    klass = unit_of % N_SEQ
    arrival = (jnp.take(deal_order.astype(jnp.int32), klass) * TOK_DEV + slot * unit_rows + within).astype(jnp.int32)
    xs = jnp.take(tokens_in, arrival, axis=1).astype(jnp.float32).reshape(TOKENS, D)
    dys = jnp.take(out_grad, arrival, axis=1).astype(jnp.float32).reshape(TOKENS, D)
    pos = jnp.stack([seq_positions(seq_lengths[w]) for w in range(PACKS)]).reshape(TOKENS)
    wfull = weights.astype(jnp.float32)
    gains = norm_gains.astype(jnp.float32)
    kernel = conv_kernel.astype(jnp.float32)

    def forward(wf, gf, kf, xf):
        return layer(wf, gf, kf, xf, pos)
    outs, pull = jax.vjp(forward, wfull, gains, kernel, xs)
    g_w, g_gains, g_kernel, g_x = pull(dys)
    scale = lax.rsqrt(jnp.asarray(TOKENS, jnp.float32))
    weight_grad = g_w * scale
    vector_grad = jnp.concatenate([g_gains, g_kernel], axis=0) * scale
    state_new = BETA_VEC * vector_state + (1.0 - BETA_VEC) * vector_grad * vector_grad
    vector_update = -LEARN_VEC * vector_grad * lax.rsqrt(state_new)
    out_pack = outs.astype(jnp.bfloat16).reshape(PACKS, PACK, D)
    dx_pack = g_x.astype(jnp.bfloat16).reshape(PACKS, PACK, D)
    block_out = jnp.zeros_like(out_pack).at[:, arrival].set(out_pack)
    input_grad = jnp.zeros_like(dx_pack).at[:, arrival].set(dx_pack)
    blocks = weight_grad.reshape(D // BLK, BLK, WCOLS // BLK, BLK).transpose(0, 2, 1, 3).reshape(NBLK, BLK, BLK)
    left_term = jnp.einsum('nij,nkj->nik', blocks, blocks, precision=HIGH)
    right_term = jnp.einsum('nji,njk->nik', blocks, blocks, precision=HIGH)
    stats_new = jnp.stack([BETA * kron_stats[0] + (1.0 - BETA) * left_term / BLK, BETA * kron_stats[1] + (1.0 - BETA) * right_term / BLK])
    left_mul = jnp.einsum('nij,njk->nik', kron_roots[0], blocks, precision=HIGH)
    update = -LEARN * jnp.einsum('nij,njk->nik', left_mul, kron_roots[1], precision=HIGH)
    return (block_out, input_grad, weight_grad, vector_grad, state_new, vector_update, stats_new, update)
```

```python
import functools

import jax
import jax.numpy as jnp
from jax import lax
from jax.experimental import pallas as pl
from jax.experimental.pallas import tpu as pltpu
from jax.sharding import PartitionSpec as P

MESH = pl.DeviceIdType.MESH

D = 1024
FF = 4608
BLK = 128


EPS = 1e-05
BETA = 0.5
BETA_VEC = 0.5
LEARN = 0.03
LEARN_VEC = 0.05
HIGH = lax.Precision.HIGHEST


def passed_along(block, axis, distance):
    devices = range(lax.axis_size(axis))
    route = [(i - distance, i) for i in devices if i - distance in devices]
    return lax.ppermute(block, axis, route)


def seq_positions(lengths_row, first, count):
    starts = jnp.cumsum(lengths_row) - lengths_row
    rows_at = first + jnp.arange(count, dtype=jnp.int32)
    begin = jnp.max(jnp.where(starts[None, :] <= rows_at[:, None], starts[None, :], 0), axis=1)
    return rows_at - begin


def rms_scale(values):
    return lax.rsqrt(jnp.mean(values * values, axis=1, keepdims=True) + EPS)


def norm_back(upstream, values, scale, gain):
    scaled = upstream * gain
    inner = jnp.mean(scaled * values, axis=1, keepdims=True)
    return (
        scale * scaled - values * scale * scale * scale * inner,
        jnp.sum(upstream * values * scale, axis=0),
    )


def contract_rows(left, right):
    return lax.dot_general(
        left, right, (((0,), (0,)), ((), ())), preferred_element_type=jnp.float32
    )


def contract_cols(left, right):
    return lax.dot_general(
        left, right, (((1,), (1,)), ((), ())), preferred_element_type=jnp.float32
    )


def plain_shards(
    tokens_in,
    out_grad,
    deal_order,
    seq_lengths,
    weights,
    norm_gains,
    conv_kernel,
    vector_state,
    kron_stats,
    kron_roots,
):
    n_seq = lax.axis_size("seq")
    n_wsh = lax.axis_size("wsh")
    rows = tokens_in.shape[1]
    unit = rows // n_seq
    arrived = (
        lax.all_to_all(
            tokens_in.reshape(n_seq, unit, D), "seq", split_axis=0, concat_axis=0, tiled=True
        ),
        lax.all_to_all(
            out_grad.reshape(n_seq, unit, D), "seq", split_axis=0, concat_axis=0, tiled=True
        ),
    )
    x_bf = jnp.take(arrived[0], deal_order, axis=0).reshape(rows, D)
    dy_bf = jnp.take(arrived[1], deal_order, axis=0).reshape(rows, D)
    full_w, gains_bf, kernel_bf = (
        lax.all_gather(weights, "wsh", axis=0, tiled=True),
        lax.all_gather(norm_gains, "wsh", axis=1, tiled=True),
        lax.all_gather(conv_kernel, "wsh", axis=1, tiled=True),
    )
    gains = gains_bf.astype(jnp.float32)
    kernel = kernel_bf.astype(jnp.float32)
    first_row = lax.axis_index("seq") * rows
    pos = seq_positions(seq_lengths[0], first_row, rows + 2)
    masks = [(pos >= 2 - k).astype(jnp.float32)[:, None] for k in range(3)]
    xf = x_bf.astype(jnp.float32)
    scale_one = rms_scale(xf)
    xn = (xf * scale_one * gains[0]).astype(jnp.bfloat16)
    proj = jnp.dot(xn, full_w[:, : 3 * D], preferred_element_type=jnp.float32)
    b_part = proj[:, :D]
    c_part = proj[:, D : 2 * D]
    x_part = proj[:, 2 * D :]
    conv_in = b_part * x_part
    prev = passed_along(conv_in[rows - 2 :], "seq", 1)
    ext = jnp.concatenate([prev, conv_in], axis=0)
    conv = (
        kernel[0] * masks[0][:rows] * ext[0:rows]
        + kernel[1] * masks[1][:rows] * ext[1 : rows + 1]
        + kernel[2] * masks[2][:rows] * ext[2 : rows + 2]
    )
    yc = (c_part * conv).astype(jnp.bfloat16)
    hidden_sum = xf + jnp.dot(yc, full_w[:, 3 * D : 4 * D], preferred_element_type=jnp.float32)
    scale_two = rms_scale(hidden_sum)
    hn = (hidden_sum * scale_two * gains[1]).astype(jnp.bfloat16)
    gate_up = jnp.dot(hn, full_w[:, 4 * D : 4 * D + 2 * FF], preferred_element_type=jnp.float32)
    gate = gate_up[:, :FF]
    upper = gate_up[:, FF:]
    sig = jax.nn.sigmoid(gate)
    act = (gate * sig * upper).astype(jnp.bfloat16)
    ffn = contract_cols(act, full_w[:, 4 * D + 2 * FF :])
    result = (hidden_sum + ffn).astype(jnp.bfloat16)
    g_down = contract_rows(dy_bf, act)
    d_act = jnp.dot(dy_bf, full_w[:, 4 * D + 2 * FF :], preferred_element_type=jnp.float32)
    d_gate = d_act * upper * sig * (1.0 + gate * (1.0 - sig))
    d_upper = d_act * gate * sig
    d_gu = jnp.concatenate([d_gate, d_upper], axis=1).astype(jnp.bfloat16)
    g_gu = contract_rows(hn, d_gu)
    d_hn = contract_cols(d_gu, full_w[:, 4 * D : 4 * D + 2 * FF])
    d_norm_two, g_gain_two = norm_back(d_hn, hidden_sum, scale_two, gains[1])
    d_hidden = dy_bf.astype(jnp.float32) + d_norm_two
    d_mix = d_hidden.astype(jnp.bfloat16)
    g_out = contract_rows(yc, d_mix)
    d_yc = contract_cols(d_mix, full_w[:, 3 * D : 4 * D])
    d_c = d_yc * conv
    d_conv = d_yc * c_part
    after = passed_along(d_conv[:2], "seq", -1)
    d_ext = jnp.concatenate([d_conv, after], axis=0)
    weighted = [d_ext * masks[k] for k in range(3)]
    d_bx = (
        kernel[2] * weighted[2][:rows]
        + kernel[1] * weighted[1][1 : rows + 1]
        + kernel[0] * weighted[0][2 : rows + 2]
    )
    g_taps = jnp.stack([jnp.sum(weighted[k][:rows] * ext[k : k + rows], axis=0) for k in range(3)])
    d_proj = jnp.concatenate([d_bx * x_part, d_c, d_bx * b_part], axis=1).astype(jnp.bfloat16)
    g_in = contract_rows(xn, d_proj)
    d_xn = contract_cols(d_proj, full_w[:, : 3 * D])
    d_norm_one, g_gain_one = norm_back(d_xn, xf, scale_one, gains[0])
    d_input = (d_hidden + d_norm_one).astype(jnp.bfloat16)
    g_vec = jnp.concatenate([g_gain_one[None], g_gain_two[None], g_taps], axis=0)
    inverse = jnp.argsort(deal_order)
    leaving = (
        jnp.take(result.reshape(n_seq, unit, D), inverse, axis=0),
        jnp.take(d_input.reshape(n_seq, unit, D), inverse, axis=0),
    )
    returned = (
        lax.all_to_all(leaving[0], "seq", split_axis=0, concat_axis=0, tiled=True),
        lax.all_to_all(leaving[1], "seq", split_axis=0, concat_axis=0, tiled=True),
    )
    summed = (
        lax.psum_scatter(g_in.astype(jnp.bfloat16), "wsh", scatter_dimension=0, tiled=True).astype(
            jnp.float32
        ),
        lax.psum_scatter(g_out.astype(jnp.bfloat16), "wsh", scatter_dimension=0, tiled=True).astype(
            jnp.float32
        ),
        lax.psum_scatter(g_gu.astype(jnp.bfloat16), "wsh", scatter_dimension=0, tiled=True).astype(
            jnp.float32
        ),
        lax.psum_scatter(
            g_down.astype(jnp.bfloat16), "wsh", scatter_dimension=0, tiled=True
        ).astype(jnp.float32),
        lax.psum_scatter(g_vec.astype(jnp.bfloat16), "wsh", scatter_dimension=1, tiled=True).astype(
            jnp.float32
        ),
    )
    summed = (
        lax.psum(summed[0].astype(jnp.bfloat16), "seq").astype(jnp.float32),
        lax.psum(summed[1].astype(jnp.bfloat16), "seq").astype(jnp.float32),
        lax.psum(summed[2].astype(jnp.bfloat16), "seq").astype(jnp.float32),
        lax.psum(summed[3].astype(jnp.bfloat16), "seq").astype(jnp.float32),
        lax.psum(summed[4].astype(jnp.bfloat16), "seq").astype(jnp.float32),
    )
    grad_scale = lax.rsqrt(jnp.asarray(rows * n_seq * n_wsh, jnp.float32))
    grad_shard = jnp.concatenate([summed[0], summed[1], summed[2], summed[3]], axis=1) * grad_scale
    vec_grad = summed[4] * grad_scale
    state_new = BETA_VEC * vector_state + (1.0 - BETA_VEC) * vec_grad * vec_grad
    vec_update = -LEARN_VEC * vec_grad * lax.rsqrt(state_new)
    nrow_blocks = grad_shard.shape[0] // BLK
    ncol_blocks = grad_shard.shape[1] // BLK
    grad_blocks = (
        grad_shard.reshape(nrow_blocks, BLK, ncol_blocks, BLK)
        .transpose(0, 2, 1, 3)
        .reshape(nrow_blocks * ncol_blocks, BLK, BLK)
    )
    share = BLK // n_seq
    first_block_row = lax.axis_index("seq") * share
    block_rows = lax.dynamic_slice_in_dim(grad_blocks, first_block_row, share, 1)
    block_cols = lax.dynamic_slice_in_dim(grad_blocks, first_block_row, share, 2)
    left_term = jnp.einsum("nij,nkj->nik", block_rows, grad_blocks, precision=HIGH)
    right_term = jnp.einsum("nji,njk->nik", block_cols, grad_blocks, precision=HIGH)
    stats_new = jnp.stack(
        [
            BETA * kron_stats[0] + (1.0 - BETA) * left_term / BLK,
            BETA * kron_stats[1] + (1.0 - BETA) * right_term / BLK,
        ]
    )
    right_full = lax.all_gather(
        kron_roots[1].astype(jnp.bfloat16), "seq", axis=1, tiled=True
    ).astype(jnp.float32)
    left_mul = jnp.einsum("nij,njk->nik", kron_roots[0], grad_blocks, precision=HIGH)
    update = -LEARN * jnp.einsum("nij,njk->nik", left_mul, right_full, precision=HIGH)
    return (
        returned[0].reshape(1, rows, D),
        returned[1].reshape(1, rows, D),
        grad_shard,
        vec_grad,
        state_new,
        vec_update,
        stats_new,
        update,
    )


COLS = 256
GAP = 2
RING = 12
SEMS = 4


def place():
    seq, wsh = lax.axis_index("seq"), lax.axis_index("wsh")
    return seq // 2, seq % 2, wsh // 2, wsh % 2


def reduce_kernel(
    edges,
    scale,
    lefts_ref,
    d_in_ref,
    d_mix_ref,
    d_gu_ref,
    act_ref,
    vec_ref,
    roots_l_ref,
    roots_r_ref,
    leave_ref,
    grad_ref,
    terms_ref,
    arrive_ref,
    b_buf,
    g_buf,
    core_in,
    y_out,
    y_in,
    x_out,
    x_in,
    z_out,
    z_in,
    final,
    r_buf,
    t_buf,
    b_sem,
    r_sem,
    o_sem,
    t_sem,
    send_sem,
    recv_sem,
    far_send,
    far_recv,
    own_sem,
):
    z, x, y, c = place()
    seq, wsh = lax.axis_index("seq"), lax.axis_index("wsh")
    n_real = edges[-1]
    count = n_real + 1
    core_id = (seq, y * 2 + (1 - c))
    y_id = (seq, (1 - y) * 2 + c)
    x_id = (z * 2 + (1 - x), wsh)
    z_ids = [(lax.rem(z + d, 4) * 2 + x, wsh) for d in (1, 2, 3)]
    far_ids = [(lax.rem(seq + d, 8), wsh) for d in range(1, 8)]

    barrier = pltpu.get_barrier_semaphore()
    for device in [core_id, y_id] + far_ids:
        pl.semaphore_signal(barrier, inc=1, device_id=device, device_id_type=MESH)
    pl.semaphore_wait(barrier, 9)

    def far(d):
        to = far_ids[d - 1]
        return pltpu.make_async_remote_copy(
            src_ref=leave_ref.at[to[0]],
            dst_ref=arrive_ref.at[seq],
            send_sem=far_send.at[d - 1],
            recv_sem=far_recv.at[d - 1],
            device_id=to,
            device_id_type=MESH,
        )

    own = pltpu.make_async_copy(leave_ref.at[seq], arrive_ref.at[seq], own_sem)
    own.start()
    for d in range(1, 8):
        far(d).start()

    def remote(flow, n, source, target, device):
        k = lax.rem(n, SEMS)
        return pltpu.make_async_remote_copy(
            src_ref=source,
            dst_ref=target,
            send_sem=send_sem.at[flow, k],
            recv_sem=recv_sem.at[flow, k],
            device_id=device,
            device_id_type=MESH,
        )

    def core_copy(n):
        slot = lax.rem(n, RING)
        return remote(0, n, g_buf.at[slot, 1 - c], core_in.at[slot], core_id)

    def y_copy(n):
        return remote(1, n, y_out.at[lax.rem(n, SEMS)], y_in.at[lax.rem(n, RING)], y_id)

    def x_copy(n):
        return remote(2, n, x_out.at[lax.rem(n, SEMS)], x_in.at[lax.rem(n, RING)], x_id)

    def z_copy(n, d):
        slot = lax.rem(n, RING)
        return remote(
            2 + d, n, z_out.at[lax.rem(n, SEMS), d - 1], z_in.at[slot, d - 1], z_ids[d - 1]
        )

    def z_share(n, d):
        piece = final.at[lax.rem(n, RING), pl.ds(pl.multiple_of(x * 128 + z * 32, 32), 32)]
        return remote(5 + d, n, piece, piece, z_ids[d - 1])

    def x_share(n):
        piece = final.at[lax.rem(n, RING), pl.ds(pl.multiple_of(x * 128, 128), 128)]
        return remote(9, n, piece, piece, x_id)

    def b_copies(n):
        slot = lax.rem(n, SEMS)
        column = n_real - n
        for r, source in enumerate((d_in_ref, d_mix_ref, d_gu_ref, act_ref)):
            low, high = edges[r], edges[r + 1]
            at = jnp.clip(column - low, 0, high - low - 1)
            at = pl.multiple_of(at * COLS, COLS)
            copy = pltpu.make_async_copy(
                source.at[:, pl.ds(at, COLS)], b_buf.at[slot], b_sem.at[slot]
            )
            yield (column >= low) & (column < high), copy

    def r_copy(n):
        slot = lax.rem(n, SEMS)
        at = pl.multiple_of(jnp.minimum(n_real - n, n_real - 1) * 2, 2)
        return pltpu.make_async_copy(
            roots_r_ref.at[:, pl.ds(at, 2)], r_buf.at[slot], r_sem.at[slot]
        )

    def o_copy(n):
        at = pl.multiple_of((n_real - n) * COLS, COLS)
        return pltpu.make_async_copy(
            final.at[lax.rem(n, RING)], grad_ref.at[:, pl.ds(at, COLS)], o_sem.at[lax.rem(n, SEMS)]
        )

    def t_copy(n):
        slot = lax.rem(n, SEMS)
        at = pl.multiple_of(jnp.minimum(n_real - n, n_real - 1) * 2, 2)
        return pltpu.make_async_copy(
            t_buf.at[slot], terms_ref.at[:, :, pl.ds(at, 2)], t_sem.at[slot]
        )

    def wide(value):
        return value.astype(jnp.float32)

    def sum_rows(slot, first, size, with_y):
        rows = pl.ds(pl.multiple_of(first, size), size)
        total = wide(g_buf[slot, c, y, rows]) + wide(core_in[slot, y, rows])
        if with_y:
            total = total + wide(y_in[slot, rows])
        return total

    def stage_load(n):
        for wanted, copy in b_copies(n):
            pl.when(wanted)(copy.start)

    def stage_product(n):
        slot = lax.rem(n, RING)
        column = n_real - n

        @pl.when(n > 0)
        def _():
            for wanted, copy in b_copies(n):
                pl.when(wanted)(copy.wait)
            region = sum((column >= e).astype(jnp.int32) for e in edges[1:-1])
            right = b_buf[lax.rem(n, SEMS)]
            for w in range(4):
                product = jnp.dot(
                    lefts_ref[region, w * 256 : (w + 1) * 256, :],
                    right,
                    preferred_element_type=jnp.float32,
                )
                g_buf[slot, w % 2, w // 2] = product.astype(jnp.bfloat16)

        @pl.when(n == 0)
        def _():
            for w in range(4):
                g_buf[slot, w % 2, w // 2] = vec_ref[w]

        core_copy(n).start()

    def stage_y(n):
        slot = lax.rem(n, RING)
        core_copy(n).wait()
        y_out[lax.rem(n, SEMS)] = (
            wide(g_buf[slot, c, 1 - y]) + wide(core_in[slot, 1 - y])
        ).astype(jnp.bfloat16)
        y_copy(n).start()

    def stage_x(n):
        slot = lax.rem(n, RING)
        y_copy(n).wait()
        x_out[lax.rem(n, SEMS)] = sum_rows(slot, (1 - x) * 128, 128, True).astype(jnp.bfloat16)
        x_copy(n).start()

    def stage_z(n):
        slot = lax.rem(n, RING)
        x_copy(n).wait()
        for d in (1, 2, 3):
            row = lax.rem(z + d, 4) * 32
            total = sum_rows(slot, x * 128 + row, 32, True)
            total = total + wide(x_in[slot, pl.ds(pl.multiple_of(row, 32), 32)])
            z_out[lax.rem(n, SEMS), d - 1] = total.astype(jnp.bfloat16)
            z_copy(n, d).start()

    def stage_final(n):
        slot = lax.rem(n, RING)
        for d in (1, 2, 3):
            z_copy(n, d).wait()
        first = x * 128 + z * 32
        total = sum_rows(slot, first, 32, True)
        total = total + wide(x_in[slot, pl.ds(pl.multiple_of(z * 32, 32), 32)])
        for d in range(3):
            total = total + wide(z_in[slot, d])
        final[slot, pl.ds(pl.multiple_of(first, 32), 32)] = (total * scale).astype(jnp.bfloat16)
        for d in (1, 2, 3):
            z_share(n, d).start()

    def stage_share(n):
        for d in (1, 2, 3):
            z_share(n, d).wait()
        x_share(n).start()
        pl.when(n > 0)(r_copy(n).start)

    def stage_take(n):
        x_share(n).wait()
        o_copy(n).start()

    def stage_use(n):
        slot = lax.rem(n, RING)
        part = lax.rem(n, SEMS)

        @pl.when(n > SEMS)
        def _():
            t_copy(n - SEMS).wait()

        @pl.when(n > 0)
        def _():
            r_copy(n).wait()
            picked = lax.broadcasted_iota(jnp.int32, (16, BLK), 1) == (
                lax.broadcasted_iota(jnp.int32, (16, BLK), 0) + seq * 16
            )
            one_hot = picked.astype(jnp.float32).astype(jnp.bfloat16)
            column = (n_real - n) * 2
            for i in range(2):
                for j in range(2):
                    lanes = slice(j * BLK, (j + 1) * BLK)
                    block = final[slot, i * BLK : (i + 1) * BLK, lanes]
                    rows = final[
                        slot, pl.ds(pl.multiple_of(i * BLK + seq * 16, 16), 16), lanes
                    ]
                    first = contract_cols(jnp.concatenate([rows, one_hot], axis=0), block)
                    turned = first[16:].astype(jnp.bfloat16)
                    second = jnp.dot(
                        jnp.concatenate([turned, roots_l_ref[i, column + j]], axis=0),
                        block,
                        preferred_element_type=jnp.float32,
                    )
                    third = jnp.dot(
                        second[16:].astype(jnp.bfloat16),
                        r_buf[part, i, j],
                        preferred_element_type=jnp.float32,
                    )
                    t_buf[part, 0, i, j] = first[:16].astype(jnp.bfloat16)
                    t_buf[part, 1, i, j] = second[:16].astype(jnp.bfloat16)
                    t_buf[part, 2, i, j] = third.astype(jnp.bfloat16)
            t_copy(n).start()

    def stage_done(n):
        o_copy(n).wait()

    offsets = {
        "load": 0,
        "product": GAP,
        "y": 2 * GAP,
        "x": 3 * GAP,
        "z": 4 * GAP,
        "final": 5 * GAP,
        "share": 6 * GAP,
        "take": 7 * GAP,
        "use": 7 * GAP,
        "done": 8 * GAP,
    }
    stages = (
        ("done", stage_done),
        ("take", stage_take),
        ("share", stage_share),
        ("final", stage_final),
        ("z", stage_z),
        ("x", stage_x),
        ("y", stage_y),
        ("product", stage_product),
        ("load", stage_load),
        ("use", stage_use),
    )

    def step(t, carry):
        for name, stage in stages:
            n = t - offsets[name]
            pl.when((n >= 0) & (n < count))(functools.partial(stage, n))
        return carry

    lax.fori_loop(0, count + offsets["done"], step, 0)
    for n in range(count - SEMS, count):
        t_copy(n).wait()
    own.wait()
    for d in range(1, 8):
        far(d).wait()


def reduced(lefts, rights, vec, roots_l, roots_r, leaving, scale):
    edges = [0]
    for right in rights:
        edges.append(edges[-1] + right.shape[1] // COLS)
    rows = rights[0].shape[0]
    count = edges[-1]
    bf16 = jnp.bfloat16
    anywhere = pl.BlockSpec(memory_space=pl.ANY)
    vmem = pl.BlockSpec(memory_space=pltpu.VMEM)
    return pl.pallas_call(
        functools.partial(reduce_kernel, tuple(edges), scale),
        out_shape=(
            jax.ShapeDtypeStruct((256, (count + 1) * COLS), bf16),
            jax.ShapeDtypeStruct((3, 2, count * 2, 16, BLK), bf16),
            jax.ShapeDtypeStruct(leaving.shape, bf16),
        ),
        in_specs=[vmem, anywhere, anywhere, anywhere, anywhere, vmem, vmem, anywhere, anywhere],
        out_specs=(anywhere, anywhere, anywhere),
        scratch_shapes=[
            pltpu.VMEM((SEMS, rows, COLS), bf16),
            pltpu.VMEM((RING, 2, 2, 256, COLS), bf16),
            pltpu.VMEM((RING, 2, 256, COLS), bf16),
            pltpu.VMEM((SEMS, 256, COLS), bf16),
            pltpu.VMEM((RING, 256, COLS), bf16),
            pltpu.VMEM((SEMS, 128, COLS), bf16),
            pltpu.VMEM((RING, 128, COLS), bf16),
            pltpu.VMEM((SEMS, 3, 32, COLS), bf16),
            pltpu.VMEM((RING, 3, 32, COLS), bf16),
            pltpu.VMEM((RING, 256, COLS), bf16),
            pltpu.VMEM((SEMS, 2, 2, BLK, BLK), bf16),
            pltpu.VMEM((SEMS, 3, 2, 2, 16, BLK), bf16),
            pltpu.SemaphoreType.DMA((SEMS,)),
            pltpu.SemaphoreType.DMA((SEMS,)),
            pltpu.SemaphoreType.DMA((SEMS,)),
            pltpu.SemaphoreType.DMA((SEMS,)),
            pltpu.SemaphoreType.DMA((10, SEMS)),
            pltpu.SemaphoreType.DMA((10, SEMS)),
            pltpu.SemaphoreType.DMA((7,)),
            pltpu.SemaphoreType.DMA((7,)),
            pltpu.SemaphoreType.DMA,
        ],
        compiler_params=pltpu.CompilerParams(
            collective_id=0, has_side_effects=True, vmem_limit_bytes=48 << 20
        ),
        cost_estimate=pl.CostEstimate(
            flops=2 * rows * 1024 * count * COLS, bytes_accessed=10**9, transcendentals=0
        ),
        name="reduce_chunks",
    )(lefts, *rights, vec, roots_l, roots_r, leaving)


def shards(
    tokens_in,
    out_grad,
    deal_order,
    seq_lengths,
    weights,
    norm_gains,
    conv_kernel,
    vector_state,
    kron_stats,
    kron_roots,
):
    n_seq = lax.axis_size("seq")
    n_wsh = lax.axis_size("wsh")
    rows = tokens_in.shape[1]
    unit = rows // n_seq
    arrived = (
        lax.all_to_all(
            tokens_in.reshape(n_seq, unit, D), "seq", split_axis=0, concat_axis=0, tiled=True
        ),
        lax.all_to_all(
            out_grad.reshape(n_seq, unit, D), "seq", split_axis=0, concat_axis=0, tiled=True
        ),
    )
    x_bf = jnp.take(arrived[0], deal_order, axis=0).reshape(rows, D)
    dy_bf = jnp.take(arrived[1], deal_order, axis=0).reshape(rows, D)
    full_w, gains_bf, kernel_bf = (
        lax.all_gather(weights, "wsh", axis=0, tiled=True),
        lax.all_gather(norm_gains, "wsh", axis=1, tiled=True),
        lax.all_gather(conv_kernel, "wsh", axis=1, tiled=True),
    )
    gains = gains_bf.astype(jnp.float32)
    kernel = kernel_bf.astype(jnp.float32)
    first_row = lax.axis_index("seq") * rows
    pos = seq_positions(seq_lengths[0], first_row, rows + 2)
    masks = [(pos >= 2 - k).astype(jnp.float32)[:, None] for k in range(3)]
    xf = x_bf.astype(jnp.float32)
    scale_one = rms_scale(xf)
    xn = (xf * scale_one * gains[0]).astype(jnp.bfloat16)
    proj = jnp.dot(xn, full_w[:, : 3 * D], preferred_element_type=jnp.float32)
    b_part = proj[:, :D]
    c_part = proj[:, D : 2 * D]
    x_part = proj[:, 2 * D :]
    conv_in = b_part * x_part
    prev = passed_along(conv_in[rows - 2 :], "seq", 1)
    ext = jnp.concatenate([prev, conv_in], axis=0)
    conv = (
        kernel[0] * masks[0][:rows] * ext[0:rows]
        + kernel[1] * masks[1][:rows] * ext[1 : rows + 1]
        + kernel[2] * masks[2][:rows] * ext[2 : rows + 2]
    )
    yc = (c_part * conv).astype(jnp.bfloat16)
    hidden_sum = xf + jnp.dot(yc, full_w[:, 3 * D : 4 * D], preferred_element_type=jnp.float32)
    scale_two = rms_scale(hidden_sum)
    hn = (hidden_sum * scale_two * gains[1]).astype(jnp.bfloat16)
    gate_up = jnp.dot(hn, full_w[:, 4 * D : 4 * D + 2 * FF], preferred_element_type=jnp.float32)
    gate = gate_up[:, :FF]
    upper = gate_up[:, FF:]
    sig = jax.nn.sigmoid(gate)
    act = (gate * sig * upper).astype(jnp.bfloat16)
    ffn = contract_cols(act, full_w[:, 4 * D + 2 * FF :])
    result = (hidden_sum + ffn).astype(jnp.bfloat16)
    d_act = jnp.dot(dy_bf, full_w[:, 4 * D + 2 * FF :], preferred_element_type=jnp.float32)
    d_gate = d_act * upper * sig * (1.0 + gate * (1.0 - sig))
    d_upper = d_act * gate * sig
    d_gu = jnp.concatenate([d_gate, d_upper], axis=1).astype(jnp.bfloat16)
    d_hn = contract_cols(d_gu, full_w[:, 4 * D : 4 * D + 2 * FF])
    d_norm_two, g_gain_two = norm_back(d_hn, hidden_sum, scale_two, gains[1])
    d_hidden = dy_bf.astype(jnp.float32) + d_norm_two
    d_mix = d_hidden.astype(jnp.bfloat16)
    d_yc = contract_cols(d_mix, full_w[:, 3 * D : 4 * D])
    d_c = d_yc * conv
    d_conv = d_yc * c_part
    after = passed_along(d_conv[:2], "seq", -1)
    d_ext = jnp.concatenate([d_conv, after], axis=0)
    weighted = [d_ext * masks[k] for k in range(3)]
    d_bx = (
        kernel[2] * weighted[2][:rows]
        + kernel[1] * weighted[1][1 : rows + 1]
        + kernel[0] * weighted[0][2 : rows + 2]
    )
    g_taps = jnp.stack([jnp.sum(weighted[k][:rows] * ext[k : k + rows], axis=0) for k in range(3)])
    d_proj = jnp.concatenate([d_bx * x_part, d_c, d_bx * b_part], axis=1).astype(jnp.bfloat16)
    d_xn = contract_cols(d_proj, full_w[:, : 3 * D])
    d_norm_one, g_gain_one = norm_back(d_xn, xf, scale_one, gains[0])
    d_input = (d_hidden + d_norm_one).astype(jnp.bfloat16)
    g_vec = jnp.concatenate([g_gain_one[None], g_gain_two[None], g_taps], axis=0)
    inverse = jnp.argsort(deal_order)
    result_leaving = jnp.take(result.reshape(n_seq, unit, D), inverse, axis=0)
    result_back = lax.all_to_all(result_leaving, "seq", split_axis=0, concat_axis=0, tiled=True)
    leaving = jnp.take(d_input.reshape(n_seq, unit, D), inverse, axis=0)
    ncol_blocks = weights.shape[1] // BLK
    nrow_blocks = weights.shape[0] // BLK
    share = BLK // n_seq
    roots_r = lax.all_gather(kron_roots[1].astype(jnp.bfloat16), "seq", axis=1, tiled=True)
    lefts = jnp.stack([xn.T, yc.T, hn.T, dy_bf.T])
    vec = jnp.pad(g_vec.T.astype(jnp.bfloat16), ((0, 0), (0, COLS - g_vec.shape[0])))
    grad_bf, terms, dx_back = reduced(
        lefts,
        (d_proj, d_mix, d_gu, act),
        vec.reshape(n_wsh, D // n_wsh, COLS),
        kron_roots[0].astype(jnp.bfloat16).reshape(nrow_blocks, ncol_blocks, share, BLK),
        roots_r.reshape(nrow_blocks, ncol_blocks, BLK, BLK),
        leaving,
        float((rows * n_seq * n_wsh) ** -0.5),
    )
    grad_shard = grad_bf[:, : weights.shape[1]].astype(jnp.float32)
    vec_grad = grad_bf[:, weights.shape[1] : weights.shape[1] + 5].astype(jnp.float32).T
    state_new = BETA_VEC * vector_state + (1.0 - BETA_VEC) * vec_grad * vec_grad
    vec_update = -LEARN_VEC * vec_grad * lax.rsqrt(state_new)
    terms = terms.reshape(3, nrow_blocks * ncol_blocks, share, BLK).astype(jnp.float32)
    stats_new = BETA * kron_stats + ((1.0 - BETA) / BLK) * terms[:2]
    return (
        result_back.reshape(1, rows, D),
        dx_back.reshape(1, rows, D),
        grad_shard,
        vec_grad,
        state_new,
        vec_update,
        stats_new,
        -LEARN * terms[2],
    )


def solution(mesh):
    known = mesh.shape["seq"] == 8 and mesh.shape["wsh"] == 4
    return jax.shard_map(
        shards if known else plain_shards,
        mesh=mesh,
        in_specs=(
            P("wsh", "seq", None),
            P("wsh", "seq", None),
            P(),
            P("wsh", None),
            P("wsh", None),
            P(None, "wsh"),
            P(None, "wsh"),
            P(None, "wsh"),
            P(None, "wsh", "seq", None),
            P(None, "wsh", "seq", None),
        ),
        out_specs=(
            P("wsh", "seq", None),
            P("wsh", "seq", None),
            P("wsh", None),
            P(None, "wsh"),
            P(None, "wsh"),
            P(None, "wsh"),
            P(None, "wsh", "seq", None),
            P("wsh", "seq", None),
        ),
        check_vma=False,
    )
```

```python
import functools

import jax
import jax.numpy as jnp
from jax import lax
from jax.experimental import pallas as pl
from jax.experimental.pallas import tpu as pltpu
from jax.sharding import PartitionSpec as P

MESH = pl.DeviceIdType.MESH

D = 1024
FF = 4608
BLK = 128


EPS = 1e-05
BETA = 0.5
BETA_VEC = 0.5
LEARN = 0.03
LEARN_VEC = 0.05
HIGH = lax.Precision.HIGHEST


def passed_along(block, axis, distance):
    devices = range(lax.axis_size(axis))
    route = [(i - distance, i) for i in devices if i - distance in devices]
    return lax.ppermute(block, axis, route)


def seq_positions(lengths_row, first, count):
    starts = jnp.cumsum(lengths_row) - lengths_row
    rows_at = first + jnp.arange(count, dtype=jnp.int32)
    begin = jnp.max(jnp.where(starts[None, :] <= rows_at[:, None], starts[None, :], 0), axis=1)
    return rows_at - begin


def rms_scale(values):
    return lax.rsqrt(jnp.mean(values * values, axis=1, keepdims=True) + EPS)


def norm_back(upstream, values, scale, gain):
    scaled = upstream * gain
    inner = jnp.mean(scaled * values, axis=1, keepdims=True)
    return (
        scale * scaled - values * scale * scale * scale * inner,
        jnp.sum(upstream * values * scale, axis=0),
    )


def contract_rows(left, right):
    return lax.dot_general(
        left, right, (((0,), (0,)), ((), ())), preferred_element_type=jnp.float32
    )


def contract_cols(left, right):
    return lax.dot_general(
        left, right, (((1,), (1,)), ((), ())), preferred_element_type=jnp.float32
    )


def plain_shards(
    tokens_in,
    out_grad,
    deal_order,
    seq_lengths,
    weights,
    norm_gains,
    conv_kernel,
    vector_state,
    kron_stats,
    kron_roots,
):
    n_seq = lax.axis_size("seq")
    n_wsh = lax.axis_size("wsh")
    rows = tokens_in.shape[1]
    unit = rows // n_seq
    arrived = (
        lax.all_to_all(
            tokens_in.reshape(n_seq, unit, D), "seq", split_axis=0, concat_axis=0, tiled=True
        ),
        lax.all_to_all(
            out_grad.reshape(n_seq, unit, D), "seq", split_axis=0, concat_axis=0, tiled=True
        ),
    )
    x_bf = jnp.take(arrived[0], deal_order, axis=0).reshape(rows, D)
    dy_bf = jnp.take(arrived[1], deal_order, axis=0).reshape(rows, D)
    full_w, gains_bf, kernel_bf = (
        lax.all_gather(weights, "wsh", axis=0, tiled=True),
        lax.all_gather(norm_gains, "wsh", axis=1, tiled=True),
        lax.all_gather(conv_kernel, "wsh", axis=1, tiled=True),
    )
    gains = gains_bf.astype(jnp.float32)
    kernel = kernel_bf.astype(jnp.float32)
    first_row = lax.axis_index("seq") * rows
    pos = seq_positions(seq_lengths[0], first_row, rows + 2)
    masks = [(pos >= 2 - k).astype(jnp.float32)[:, None] for k in range(3)]
    xf = x_bf.astype(jnp.float32)
    scale_one = rms_scale(xf)
    xn = (xf * scale_one * gains[0]).astype(jnp.bfloat16)
    proj = jnp.dot(xn, full_w[:, : 3 * D], preferred_element_type=jnp.float32)
    b_part = proj[:, :D]
    c_part = proj[:, D : 2 * D]
    x_part = proj[:, 2 * D :]
    conv_in = b_part * x_part
    prev = passed_along(conv_in[rows - 2 :], "seq", 1)
    ext = jnp.concatenate([prev, conv_in], axis=0)
    conv = (
        kernel[0] * masks[0][:rows] * ext[0:rows]
        + kernel[1] * masks[1][:rows] * ext[1 : rows + 1]
        + kernel[2] * masks[2][:rows] * ext[2 : rows + 2]
    )
    yc = (c_part * conv).astype(jnp.bfloat16)
    hidden_sum = xf + jnp.dot(yc, full_w[:, 3 * D : 4 * D], preferred_element_type=jnp.float32)
    scale_two = rms_scale(hidden_sum)
    hn = (hidden_sum * scale_two * gains[1]).astype(jnp.bfloat16)
    gate_up = jnp.dot(hn, full_w[:, 4 * D : 4 * D + 2 * FF], preferred_element_type=jnp.float32)
    gate = gate_up[:, :FF]
    upper = gate_up[:, FF:]
    sig = jax.nn.sigmoid(gate)
    act = (gate * sig * upper).astype(jnp.bfloat16)
    ffn = contract_cols(act, full_w[:, 4 * D + 2 * FF :])
    result = (hidden_sum + ffn).astype(jnp.bfloat16)
    g_down = contract_rows(dy_bf, act)
    d_act = jnp.dot(dy_bf, full_w[:, 4 * D + 2 * FF :], preferred_element_type=jnp.float32)
    d_gate = d_act * upper * sig * (1.0 + gate * (1.0 - sig))
    d_upper = d_act * gate * sig
    d_gu = jnp.concatenate([d_gate, d_upper], axis=1).astype(jnp.bfloat16)
    g_gu = contract_rows(hn, d_gu)
    d_hn = contract_cols(d_gu, full_w[:, 4 * D : 4 * D + 2 * FF])
    d_norm_two, g_gain_two = norm_back(d_hn, hidden_sum, scale_two, gains[1])
    d_hidden = dy_bf.astype(jnp.float32) + d_norm_two
    d_mix = d_hidden.astype(jnp.bfloat16)
    g_out = contract_rows(yc, d_mix)
    d_yc = contract_cols(d_mix, full_w[:, 3 * D : 4 * D])
    d_c = d_yc * conv
    d_conv = d_yc * c_part
    after = passed_along(d_conv[:2], "seq", -1)
    d_ext = jnp.concatenate([d_conv, after], axis=0)
    weighted = [d_ext * masks[k] for k in range(3)]
    d_bx = (
        kernel[2] * weighted[2][:rows]
        + kernel[1] * weighted[1][1 : rows + 1]
        + kernel[0] * weighted[0][2 : rows + 2]
    )
    g_taps = jnp.stack([jnp.sum(weighted[k][:rows] * ext[k : k + rows], axis=0) for k in range(3)])
    d_proj = jnp.concatenate([d_bx * x_part, d_c, d_bx * b_part], axis=1).astype(jnp.bfloat16)
    g_in = contract_rows(xn, d_proj)
    d_xn = contract_cols(d_proj, full_w[:, : 3 * D])
    d_norm_one, g_gain_one = norm_back(d_xn, xf, scale_one, gains[0])
    d_input = (d_hidden + d_norm_one).astype(jnp.bfloat16)
    g_vec = jnp.concatenate([g_gain_one[None], g_gain_two[None], g_taps], axis=0)
    inverse = jnp.argsort(deal_order)
    leaving = (
        jnp.take(result.reshape(n_seq, unit, D), inverse, axis=0),
        jnp.take(d_input.reshape(n_seq, unit, D), inverse, axis=0),
    )
    returned = (
        lax.all_to_all(leaving[0], "seq", split_axis=0, concat_axis=0, tiled=True),
        lax.all_to_all(leaving[1], "seq", split_axis=0, concat_axis=0, tiled=True),
    )
    summed = (
        lax.psum_scatter(g_in.astype(jnp.bfloat16), "wsh", scatter_dimension=0, tiled=True).astype(
            jnp.float32
        ),
        lax.psum_scatter(g_out.astype(jnp.bfloat16), "wsh", scatter_dimension=0, tiled=True).astype(
            jnp.float32
        ),
        lax.psum_scatter(g_gu.astype(jnp.bfloat16), "wsh", scatter_dimension=0, tiled=True).astype(
            jnp.float32
        ),
        lax.psum_scatter(
            g_down.astype(jnp.bfloat16), "wsh", scatter_dimension=0, tiled=True
        ).astype(jnp.float32),
        lax.psum_scatter(g_vec.astype(jnp.bfloat16), "wsh", scatter_dimension=1, tiled=True).astype(
            jnp.float32
        ),
    )
    summed = (
        lax.psum(summed[0].astype(jnp.bfloat16), "seq").astype(jnp.float32),
        lax.psum(summed[1].astype(jnp.bfloat16), "seq").astype(jnp.float32),
        lax.psum(summed[2].astype(jnp.bfloat16), "seq").astype(jnp.float32),
        lax.psum(summed[3].astype(jnp.bfloat16), "seq").astype(jnp.float32),
        lax.psum(summed[4].astype(jnp.bfloat16), "seq").astype(jnp.float32),
    )
    grad_scale = lax.rsqrt(jnp.asarray(rows * n_seq * n_wsh, jnp.float32))
    grad_shard = jnp.concatenate([summed[0], summed[1], summed[2], summed[3]], axis=1) * grad_scale
    vec_grad = summed[4] * grad_scale
    state_new = BETA_VEC * vector_state + (1.0 - BETA_VEC) * vec_grad * vec_grad
    vec_update = -LEARN_VEC * vec_grad * lax.rsqrt(state_new)
    nrow_blocks = grad_shard.shape[0] // BLK
    ncol_blocks = grad_shard.shape[1] // BLK
    grad_blocks = (
        grad_shard.reshape(nrow_blocks, BLK, ncol_blocks, BLK)
        .transpose(0, 2, 1, 3)
        .reshape(nrow_blocks * ncol_blocks, BLK, BLK)
    )
    share = BLK // n_seq
    first_block_row = lax.axis_index("seq") * share
    block_rows = lax.dynamic_slice_in_dim(grad_blocks, first_block_row, share, 1)
    block_cols = lax.dynamic_slice_in_dim(grad_blocks, first_block_row, share, 2)
    left_term = jnp.einsum("nij,nkj->nik", block_rows, grad_blocks, precision=HIGH)
    right_term = jnp.einsum("nji,njk->nik", block_cols, grad_blocks, precision=HIGH)
    stats_new = jnp.stack(
        [
            BETA * kron_stats[0] + (1.0 - BETA) * left_term / BLK,
            BETA * kron_stats[1] + (1.0 - BETA) * right_term / BLK,
        ]
    )
    right_full = lax.all_gather(
        kron_roots[1].astype(jnp.bfloat16), "seq", axis=1, tiled=True
    ).astype(jnp.float32)
    left_mul = jnp.einsum("nij,njk->nik", kron_roots[0], grad_blocks, precision=HIGH)
    update = -LEARN * jnp.einsum("nij,njk->nik", left_mul, right_full, precision=HIGH)
    return (
        returned[0].reshape(1, rows, D),
        returned[1].reshape(1, rows, D),
        grad_shard,
        vec_grad,
        state_new,
        vec_update,
        stats_new,
        update,
    )


COLS = 256
GAP = 2
RING = 12
SEMS = 4


def place():
    seq, wsh = lax.axis_index("seq"), lax.axis_index("wsh")
    return seq // 2, seq % 2, wsh // 2, wsh % 2


def reduce_kernel(
    edges,
    scale,
    lefts_ref,
    d_in_ref,
    d_mix_ref,
    d_gu_ref,
    act_ref,
    vec_ref,
    roots_l_ref,
    roots_r_ref,
    leave_ref,
    grad_ref,
    terms_ref,
    arrive_ref,
    b_buf,
    g_buf,
    core_in,
    y_out,
    y_in,
    x_out,
    x_in,
    z_out,
    z_in,
    final,
    r_buf,
    t_buf,
    b_sem,
    r_sem,
    o_sem,
    t_sem,
    send_sem,
    recv_sem,
    far_send,
    far_recv,
    own_sem,
):
    z, x, y, c = place()
    seq, wsh = lax.axis_index("seq"), lax.axis_index("wsh")
    n_real = edges[-1]
    count = n_real + 1
    core_id = (seq, y * 2 + (1 - c))
    y_id = (seq, (1 - y) * 2 + c)
    x_id = (z * 2 + (1 - x), wsh)
    z_ids = [(lax.rem(z + d, 4) * 2 + x, wsh) for d in (1, 2, 3)]
    far_ids = [(lax.rem(seq + d, 8), wsh) for d in range(1, 8)]

    barrier = pltpu.get_barrier_semaphore()
    for device in [core_id, y_id] + far_ids:
        pl.semaphore_signal(barrier, inc=1, device_id=device, device_id_type=MESH)
    pl.semaphore_wait(barrier, 9)

    def far(d):
        to = far_ids[d - 1]
        return pltpu.make_async_remote_copy(
            src_ref=leave_ref.at[to[0]],
            dst_ref=arrive_ref.at[seq],
            send_sem=far_send.at[d - 1],
            recv_sem=far_recv.at[d - 1],
            device_id=to,
            device_id_type=MESH,
        )

    own = pltpu.make_async_copy(leave_ref.at[seq], arrive_ref.at[seq], own_sem)
    own.start()
    for d in range(1, 8):
        far(d).start()

    def remote(flow, n, source, target, device):
        k = lax.rem(n, SEMS)
        return pltpu.make_async_remote_copy(
            src_ref=source,
            dst_ref=target,
            send_sem=send_sem.at[flow, k],
            recv_sem=recv_sem.at[flow, k],
            device_id=device,
            device_id_type=MESH,
        )

    def core_copy(n):
        slot = lax.rem(n, RING)
        return remote(0, n, g_buf.at[slot, 1 - c], core_in.at[slot], core_id)

    def y_copy(n):
        return remote(1, n, y_out.at[lax.rem(n, SEMS)], y_in.at[lax.rem(n, RING)], y_id)

    def x_copy(n):
        return remote(2, n, x_out.at[lax.rem(n, SEMS)], x_in.at[lax.rem(n, RING)], x_id)

    def z_copy(n, d):
        slot = lax.rem(n, RING)
        return remote(
            2 + d, n, z_out.at[lax.rem(n, SEMS), d - 1], z_in.at[slot, d - 1], z_ids[d - 1]
        )

    def z_share(n, d):
        piece = final.at[lax.rem(n, RING), pl.ds(pl.multiple_of(x * 128 + z * 32, 32), 32)]
        return remote(5 + d, n, piece, piece, z_ids[d - 1])

    def x_share(n):
        piece = final.at[lax.rem(n, RING), pl.ds(pl.multiple_of(x * 128, 128), 128)]
        return remote(9, n, piece, piece, x_id)

    def b_copies(n):
        slot = lax.rem(n, SEMS)
        column = n_real - n
        for r, source in enumerate((d_in_ref, d_mix_ref, d_gu_ref, act_ref)):
            low, high = edges[r], edges[r + 1]
            at = jnp.clip(column - low, 0, high - low - 1)
            at = pl.multiple_of(at * COLS, COLS)
            copy = pltpu.make_async_copy(
                source.at[:, pl.ds(at, COLS)], b_buf.at[slot], b_sem.at[slot]
            )
            yield (column >= low) & (column < high), copy

    def r_copy(n):
        slot = lax.rem(n, SEMS)
        at = pl.multiple_of(jnp.minimum(n_real - n, n_real - 1) * 2, 2)
        return pltpu.make_async_copy(
            roots_r_ref.at[:, pl.ds(at, 2)], r_buf.at[slot], r_sem.at[slot]
        )

    def o_copy(n):
        at = pl.multiple_of((n_real - n) * COLS, COLS)
        return pltpu.make_async_copy(
            final.at[lax.rem(n, RING)], grad_ref.at[:, pl.ds(at, COLS)], o_sem.at[lax.rem(n, SEMS)]
        )

    def t_copy(n):
        slot = lax.rem(n, SEMS)
        at = pl.multiple_of(jnp.minimum(n_real - n, n_real - 1) * 2, 2)
        return pltpu.make_async_copy(
            t_buf.at[slot], terms_ref.at[:, :, pl.ds(at, 2)], t_sem.at[slot]
        )

    def wide(value):
        return value.astype(jnp.float32)

    def sum_rows(slot, first, size, with_y):
        rows = pl.ds(pl.multiple_of(first, size), size)
        total = wide(g_buf[slot, c, y, rows]) + wide(core_in[slot, y, rows])
        if with_y:
            total = total + wide(y_in[slot, rows])
        return total

    def stage_load(n):
        for wanted, copy in b_copies(n):
            pl.when(wanted)(copy.start)

    def stage_product(n):
        slot = lax.rem(n, RING)
        column = n_real - n

        @pl.when(n > 0)
        def _():
            for wanted, copy in b_copies(n):
                pl.when(wanted)(copy.wait)
            region = sum((column >= e).astype(jnp.int32) for e in edges[1:-1])
            right = b_buf[lax.rem(n, SEMS)]
            for w in range(4):
                product = jnp.dot(
                    lefts_ref[region, w * 256 : (w + 1) * 256, :],
                    right,
                    preferred_element_type=jnp.float32,
                )
                g_buf[slot, w % 2, w // 2] = product.astype(jnp.bfloat16)

        @pl.when(n == 0)
        def _():
            for w in range(4):
                g_buf[slot, w % 2, w // 2] = vec_ref[w]

        core_copy(n).start()

    def stage_y(n):
        slot = lax.rem(n, RING)
        core_copy(n).wait()
        y_out[lax.rem(n, SEMS)] = (
            wide(g_buf[slot, c, 1 - y]) + wide(core_in[slot, 1 - y])
        ).astype(jnp.bfloat16)
        y_copy(n).start()

    def stage_x(n):
        slot = lax.rem(n, RING)
        y_copy(n).wait()
        x_out[lax.rem(n, SEMS)] = sum_rows(slot, (1 - x) * 128, 128, True).astype(jnp.bfloat16)
        x_copy(n).start()

    def stage_z(n):
        slot = lax.rem(n, RING)
        x_copy(n).wait()
        for d in (1, 2, 3):
            row = lax.rem(z + d, 4) * 32
            total = sum_rows(slot, x * 128 + row, 32, True)
            total = total + wide(x_in[slot, pl.ds(pl.multiple_of(row, 32), 32)])
            z_out[lax.rem(n, SEMS), d - 1] = total.astype(jnp.bfloat16)
            z_copy(n, d).start()

    def stage_final(n):
        slot = lax.rem(n, RING)
        for d in (1, 2, 3):
            z_copy(n, d).wait()
        first = x * 128 + z * 32
        total = sum_rows(slot, first, 32, True)
        total = total + wide(x_in[slot, pl.ds(pl.multiple_of(z * 32, 32), 32)])
        for d in range(3):
            total = total + wide(z_in[slot, d])
        final[slot, pl.ds(pl.multiple_of(first, 32), 32)] = (total * scale).astype(jnp.bfloat16)
        for d in (1, 2, 3):
            z_share(n, d).start()

    def stage_share(n):
        for d in (1, 2, 3):
            z_share(n, d).wait()
        x_share(n).start()
        pl.when(n > 0)(r_copy(n).start)

    def stage_take(n):
        x_share(n).wait()
        o_copy(n).start()

    def stage_use(n):
        slot = lax.rem(n, RING)
        part = lax.rem(n, SEMS)

        @pl.when(n > SEMS)
        def _():
            t_copy(n - SEMS).wait()

        @pl.when(n > 0)
        def _():
            r_copy(n).wait()
            picked = lax.broadcasted_iota(jnp.int32, (16, BLK), 1) == (
                lax.broadcasted_iota(jnp.int32, (16, BLK), 0) + seq * 16
            )
            one_hot = picked.astype(jnp.float32).astype(jnp.bfloat16)
            column = (n_real - n) * 2
            for i in range(2):
                for j in range(2):
                    lanes = slice(j * BLK, (j + 1) * BLK)
                    block = final[slot, i * BLK : (i + 1) * BLK, lanes]
                    rows = final[
                        slot, pl.ds(pl.multiple_of(i * BLK + seq * 16, 16), 16), lanes
                    ]
                    first = contract_cols(jnp.concatenate([rows, one_hot], axis=0), block)
                    turned = first[16:].astype(jnp.bfloat16)
                    second = jnp.dot(
                        jnp.concatenate([turned, roots_l_ref[i, column + j]], axis=0),
                        block,
                        preferred_element_type=jnp.float32,
                    )
                    third = jnp.dot(
                        second[16:].astype(jnp.bfloat16),
                        r_buf[part, i, j],
                        preferred_element_type=jnp.float32,
                    )
                    t_buf[part, 0, i, j] = first[:16].astype(jnp.bfloat16)
                    t_buf[part, 1, i, j] = second[:16].astype(jnp.bfloat16)
                    t_buf[part, 2, i, j] = third.astype(jnp.bfloat16)
            t_copy(n).start()

    def stage_done(n):
        o_copy(n).wait()

    offsets = {
        "load": 0,
        "product": GAP,
        "y": 2 * GAP,
        "x": 3 * GAP,
        "z": 4 * GAP,
        "final": 5 * GAP,
        "share": 6 * GAP,
        "take": 7 * GAP,
        "use": 7 * GAP,
        "done": 8 * GAP,
    }
    stages = (
        ("done", stage_done),
        ("take", stage_take),
        ("share", stage_share),
        ("final", stage_final),
        ("z", stage_z),
        ("x", stage_x),
        ("y", stage_y),
        ("product", stage_product),
        ("load", stage_load),
        ("use", stage_use),
    )

    def step(t, carry):
        for name, stage in stages:
            n = t - offsets[name]
            pl.when((n >= 0) & (n < count))(functools.partial(stage, n))
        return carry

    lax.fori_loop(0, count + offsets["done"], step, 0)
    for n in range(count - SEMS, count):
        t_copy(n).wait()
    own.wait()
    for d in range(1, 8):
        far(d).wait()


def reduced(lefts, rights, vec, roots_l, roots_r, leaving, scale):
    edges = [0]
    for right in rights:
        edges.append(edges[-1] + right.shape[1] // COLS)
    rows = rights[0].shape[0]
    count = edges[-1]
    bf16 = jnp.bfloat16
    anywhere = pl.BlockSpec(memory_space=pl.ANY)
    vmem = pl.BlockSpec(memory_space=pltpu.VMEM)
    return pl.pallas_call(
        functools.partial(reduce_kernel, tuple(edges), scale),
        out_shape=(
            jax.ShapeDtypeStruct((256, (count + 1) * COLS), bf16),
            jax.ShapeDtypeStruct((3, 2, count * 2, 16, BLK), bf16),
            jax.ShapeDtypeStruct(leaving.shape, bf16),
        ),
        in_specs=[vmem, anywhere, anywhere, anywhere, anywhere, vmem, vmem, anywhere, anywhere],
        out_specs=(anywhere, anywhere, anywhere),
        scratch_shapes=[
            pltpu.VMEM((SEMS, rows, COLS), bf16),
            pltpu.VMEM((RING, 2, 2, 256, COLS), bf16),
            pltpu.VMEM((RING, 2, 256, COLS), bf16),
            pltpu.VMEM((SEMS, 256, COLS), bf16),
            pltpu.VMEM((RING, 256, COLS), bf16),
            pltpu.VMEM((SEMS, 128, COLS), bf16),
            pltpu.VMEM((RING, 128, COLS), bf16),
            pltpu.VMEM((SEMS, 3, 32, COLS), bf16),
            pltpu.VMEM((RING, 3, 32, COLS), bf16),
            pltpu.VMEM((RING, 256, COLS), bf16),
            pltpu.VMEM((SEMS, 2, 2, BLK, BLK), bf16),
            pltpu.VMEM((SEMS, 3, 2, 2, 16, BLK), bf16),
            pltpu.SemaphoreType.DMA((SEMS,)),
            pltpu.SemaphoreType.DMA((SEMS,)),
            pltpu.SemaphoreType.DMA((SEMS,)),
            pltpu.SemaphoreType.DMA((SEMS,)),
            pltpu.SemaphoreType.DMA((10, SEMS)),
            pltpu.SemaphoreType.DMA((10, SEMS)),
            pltpu.SemaphoreType.DMA((7,)),
            pltpu.SemaphoreType.DMA((7,)),
            pltpu.SemaphoreType.DMA,
        ],
        compiler_params=pltpu.CompilerParams(
            collective_id=0, has_side_effects=True, vmem_limit_bytes=48 << 20
        ),
        cost_estimate=pl.CostEstimate(
            flops=2 * rows * 1024 * count * COLS, bytes_accessed=10**9, transcendentals=0
        ),
        name="reduce_chunks",
    )(lefts, *rights, vec, roots_l, roots_r, leaving)


HEAD = 512
TRIO = 256
AHEAD = 6


def forward_kernel(
    deal_ref,
    tokens_ref,
    dy_ref,
    weights_ref,
    small_ref,
    masks_ref,
    lefts_ref,
    x_ref,
    dy_out_ref,
    proj_ref,
    prev_ref,
    h_ref,
    act_ref,
    d_gu_ref,
    d_hn_ref,
    result_ref,
    heads_ref,
    smalls_ref,
    x_in,
    dy_in,
    heads,
    trios,
    smalls,
    xs,
    dys,
    xn,
    yc,
    hn,
    turned,
    proj,
    mixed,
    total,
    back,
    act_buf,
    d_gu_buf,
    own_sem,
    load_sem,
    far_send,
    far_recv,
    small_send,
    small_recv,
    send_sem,
    recv_sem,
    halo_sem,
    out_sem,
    act_sem,
):
    z, x, y, c = place()
    seq, wsh = lax.axis_index("seq"), lax.axis_index("wsh")
    bf16 = jnp.bfloat16
    n_heads, n_trios = heads.shape[0], trios.shape[0]
    count = n_heads + n_trios
    core_id = (seq, y * 2 + (1 - c))
    y_id = (seq, (1 - y) * 2 + c)
    cross_id = (seq, (1 - y) * 2 + (1 - c))
    x_id = (z * 2 + (1 - x), wsh)
    z_id = ((z + 1 - 2 * (z % 2)) * 2 + x, wsh)
    far_ids = [(lax.rem(seq + d, 8), wsh) for d in range(1, 8)]
    quarter = x * 2 + z % 2
    mine = pl.multiple_of(wsh * 256, 256)
    theirs = pl.multiple_of(((1 - y) * 2 + c) * 256, 256)

    barrier = pltpu.get_barrier_semaphore()
    for device in [core_id, y_id, cross_id] + far_ids:
        pl.semaphore_signal(barrier, inc=1, device_id=device, device_id_type=MESH)
    pl.semaphore_wait(barrier, 10)

    def far(k, d, source, target):
        to = far_ids[d - 1]
        return pltpu.make_async_remote_copy(
            src_ref=source.at[to[0]],
            dst_ref=target.at[seq],
            send_sem=far_send.at[k, d - 1],
            recv_sem=far_recv.at[k, d - 1],
            device_id=to,
            device_id_type=MESH,
        )

    def small_copy(k, to):
        return pltpu.make_async_remote_copy(
            src_ref=small_ref,
            dst_ref=smalls.at[:, pl.ds(mine, 256)],
            send_sem=small_send.at[k],
            recv_sem=small_recv.at[k],
            device_id=to,
            device_id_type=MESH,
        )

    small_ids = (core_id, y_id, cross_id)
    own_copies = (
        pltpu.make_async_copy(tokens_ref.at[seq], x_in.at[seq], own_sem.at[0]),
        pltpu.make_async_copy(dy_ref.at[seq], dy_in.at[seq], own_sem.at[1]),
        pltpu.make_async_copy(small_ref, smalls.at[:, pl.ds(mine, 256)], own_sem.at[2]),
    )
    for copy in own_copies:
        copy.start()
    for d in range(1, 8):
        far(0, d, tokens_ref, x_in).start()
    for k, to in enumerate(small_ids):
        small_copy(k, to).start()

    def head_loads(u):
        at = u * HEAD if isinstance(u, int) else pl.multiple_of(u * HEAD, HEAD)
        return [
            pltpu.make_async_copy(
                weights_ref.at[:, pl.ds(at, HEAD)],
                heads.at[u, pl.ds(mine, 256)],
                load_sem.at[u],
            )
        ]

    def trio_loads(k, sem):
        first = n_heads * HEAD
        return [
            pltpu.make_async_copy(
                weights_ref.at[
                    :,
                    pl.ds(
                        pl.multiple_of(first + part * n_trios * TRIO + k * TRIO, TRIO), TRIO
                    ),
                ],
                trios.at[k, pl.ds(mine, 256), pl.ds(part * TRIO, TRIO)],
                load_sem.at[n_heads + part * n_trios + k],
            )
            for part in range(3)
        ]

    def remote(flow, buf, i, unit, first, rows, to):
        piece = buf.at[i, pl.ds(pl.multiple_of(first, rows), rows)]
        return pltpu.make_async_remote_copy(
            src_ref=piece,
            dst_ref=piece,
            send_sem=send_sem.at[flow, unit],
            recv_sem=recv_sem.at[flow, unit],
            device_id=to,
            device_id_type=MESH,
        )

    def copies(buf, i, unit):
        near = mine + quarter * 64
        wide = mine + (3 - quarter) * 64
        got = theirs + quarter * 64
        table = {
            "core": (0, mine, 256, core_id),
            "near": (1, near, 64, y_id),
            "wide": (2, wide, 64, y_id),
            "x": (3, got, 64, x_id),
            "z": (4, got, 64, z_id),
            "pass": (5, theirs, 256, core_id),
        }

        def pick(name):
            flow, first, rows, to = table[name]
            return remote(flow, buf, i, unit, first, rows, to)

        return pick

    def head(u):
        return copies(heads, u, u)

    def trio(k):
        return copies(trios, k, n_heads + k)

    def send_first(c3):
        c3("near").start()
        c3("wide").start()
        c3("core").start()

    def send_on(c3):
        c3("near").wait()
        c3("x").start()
        c3("z").start()

    def hand_over(c3):
        c3("wide").wait()
        c3("x").wait()
        c3("z").wait()
        c3("pass").start()

    def arrived(c3):
        c3("core").wait()
        c3("pass").wait()

    for u in range(n_heads):
        for copy in head_loads(u):
            copy.start()

    def load_trio(k, carry):
        for copy in trio_loads(k, None):
            copy.start()
        return carry

    lax.fori_loop(0, n_trios, load_trio, 0)
    for u in range(n_heads):
        for copy in head_loads(u):
            copy.wait()
        send_first(head(u))

    def first_trio(k):
        for copy in trio_loads(k, None):
            copy.wait()
        send_first(trio(k))

    def turn(source, r, wait):
        copy = pltpu.make_async_copy(turned, lefts_ref.at[r], out_sem.at[0])
        if wait:
            copy.wait()
        for j in range(8):
            turned[j * 128 : (j + 1) * 128, :] = source[:, j * 128 : (j + 1) * 128].T
        copy.start()

    for d in range(1, 8):
        far(0, d, tokens_ref, x_in).wait()
    own_copies[0].wait()
    for k, to in enumerate(small_ids):
        small_copy(k, to).wait()
    own_copies[2].wait()
    for d in range(1, 8):
        far(1, d, dy_ref, dy_in).start()
    gain_one = smalls[0:1, :].astype(jnp.float32)
    for k in range(8):
        rows = slice(k * 64, (k + 1) * 64)
        unit = x_in[deal_ref[k]]
        xs[rows] = unit
        value = unit.astype(jnp.float32)
        xn[rows] = (value * rms_scale(value) * gain_one).astype(bf16)
    turn(xn, 0, False)

    def mixer_unit(u):
        proj[:, u * HEAD : (u + 1) * HEAD] = jnp.dot(
            xn[...], heads[u], preferred_element_type=jnp.float32
        )

    for u in range(n_heads + 2):
        if u < n_heads:
            send_on(head(u))
        if u >= 1 and u - 1 < n_heads:
            hand_over(head(u - 1))
        if u < AHEAD:
            first_trio(u)
        if u >= 2:
            arrived(head(u - 2))
            if u - 2 < 6:
                mixer_unit(u - 2)

    out_proj = pltpu.make_async_copy(proj, proj_ref, out_sem.at[1])
    out_proj.start()
    width = D
    halo = slice(0, 8)
    for i in range(4):
        rows = slice(i * 128, (i + 1) * 128)
        back[8 + i * 128 : 8 + (i + 1) * 128] = proj[rows, :width] * proj[rows, 2 * width :]
    ring = pltpu.make_async_remote_copy(
        src_ref=back.at[pl.ds(512, 8)],
        dst_ref=mixed,
        send_sem=halo_sem.at[0],
        recv_sem=halo_sem.at[1],
        device_id=far_ids[0],
        device_id_type=MESH,
    )
    ring.start()
    send_on(trio(0))
    for d in range(1, 8):
        far(1, d, dy_ref, dy_in).wait()
    own_copies[1].wait()
    for k in range(8):
        dys[k * 64 : (k + 1) * 64] = dy_in[deal_ref[k]]
    turn(dys, 3, True)
    ring.wait()
    back[halo] = mixed[...]
    taps = [smalls[2 + k : 3 + k, :].astype(jnp.float32) for k in range(3)]
    for i in range(8):
        first = i * 64
        rows = slice(first, first + 64)
        conv = (
            taps[0] * masks_ref[0, rows] * back[first + 6 : first + 70]
            + taps[1] * masks_ref[1, rows] * back[first + 7 : first + 71]
            + taps[2] * back[first + 8 : first + 72]
        )
        yc[rows] = (proj[rows, width : 2 * width] * conv).astype(bf16)
    hand_over(trio(0))
    for u in range(6, n_heads):
        lanes = slice((u - 6) * HEAD, (u - 5) * HEAD)
        total[:, lanes] = xs[:, lanes].astype(jnp.float32) + jnp.dot(
            yc[...], heads[u], preferred_element_type=jnp.float32
        )
    out_h = pltpu.make_async_copy(total, h_ref, out_sem.at[2])
    out_h.start()
    gain_two = smalls[1:2, :].astype(jnp.float32)
    for i in range(8):
        rows = slice(i * 64, (i + 1) * 64)
        value = total[rows]
        hn[rows] = (value * rms_scale(value) * gain_two).astype(bf16)
    for i in range(4):
        back[i * 128 : (i + 1) * 128] = jnp.zeros((128, width), jnp.float32)
    send_on(trio(1))
    turn(yc, 1, True)
    out_h.wait()

    def act_copies(k, slot):
        at = pl.multiple_of(k * TRIO, TRIO)
        up = pl.multiple_of((n_trios + k) * TRIO, TRIO)
        return (
            pltpu.make_async_copy(
                act_buf.at[slot], act_ref.at[:, pl.ds(at, TRIO)], act_sem.at[slot, 0]
            ),
            pltpu.make_async_copy(
                d_gu_buf.at[slot, :, pl.ds(0, TRIO)],
                d_gu_ref.at[:, pl.ds(at, TRIO)],
                act_sem.at[slot, 1],
            ),
            pltpu.make_async_copy(
                d_gu_buf.at[slot, :, pl.ds(TRIO, TRIO)],
                d_gu_ref.at[:, pl.ds(up, TRIO)],
                act_sem.at[slot, 2],
            ),
        )

    def ffn(k, carry):
        pl.when(k + AHEAD < n_trios)(lambda: first_trio(k + AHEAD))
        pl.when(k + 2 < n_trios)(lambda: send_on(trio(k + 2)))
        pl.when(k + 1 < n_trios)(lambda: hand_over(trio(k + 1)))
        arrived(trio(k))
        slot = lax.rem(k, 2)

        @pl.when(k >= 2)
        def _():
            for copy in act_copies(k - 2, slot):
                copy.wait()

        gate = jnp.dot(hn[...], trios[k, :, :TRIO], preferred_element_type=jnp.float32)
        upper = jnp.dot(
            hn[...], trios[k, :, TRIO : 2 * TRIO], preferred_element_type=jnp.float32
        )
        d_act = jnp.dot(dys[...], trios[k, :, 2 * TRIO :], preferred_element_type=jnp.float32)
        sig = jax.nn.sigmoid(gate)
        silu = gate * sig
        act_buf[slot] = (silu * upper).astype(bf16)
        d_gu_buf[slot, :, :TRIO] = (
            d_act * upper * sig * (1.0 + gate * (1.0 - sig))
        ).astype(bf16)
        d_gu_buf[slot, :, TRIO:] = (d_act * silu).astype(bf16)
        for copy in act_copies(k, slot):
            copy.start()
        total[...] += contract_cols(act_buf[slot], trios[k, :, 2 * TRIO :])
        back[0:512] += contract_cols(d_gu_buf[slot], trios[k, :, : 2 * TRIO])
        return carry

    lax.fori_loop(0, n_trios, ffn, 0)
    turn(hn, 2, True)
    out_back = pltpu.make_async_copy(back.at[pl.ds(0, 512)], d_hn_ref, out_sem.at[3])
    out_back.start()
    yc[...] = total[...].astype(bf16)
    last = (
        pltpu.make_async_copy(yc, result_ref, out_sem.at[4]),
        pltpu.make_async_copy(xs, x_ref, out_sem.at[5]),
        pltpu.make_async_copy(dys, dy_out_ref, out_sem.at[6]),
        pltpu.make_async_copy(smalls, smalls_ref, out_sem.at[7]),
        pltpu.make_async_copy(mixed, prev_ref, out_sem.at[8]),
        pltpu.make_async_copy(heads, heads_ref, out_sem.at[9]),
    )
    for copy in last:
        copy.start()
    for k in range(n_trios - 2, n_trios):
        for copy in act_copies(k, k % 2):
            copy.wait()
    for copy in last:
        copy.wait()
    out_proj.wait()
    out_back.wait()
    pltpu.make_async_copy(turned, lefts_ref.at[2], out_sem.at[0]).wait()


def gathered_forward(deal_order, tokens, dys, weights, small, masks):
    bf16, f32 = jnp.bfloat16, jnp.float32
    rows = tokens.shape[0] * tokens.shape[1]
    n_heads = 4 * D // HEAD
    n_trios = FF // TRIO
    count = n_heads + n_trios
    anywhere = pl.BlockSpec(memory_space=pl.ANY)
    vmem = pl.BlockSpec(memory_space=pltpu.VMEM)
    shape = jax.ShapeDtypeStruct
    return pl.pallas_call(
        forward_kernel,
        out_shape=(
            shape((4, D, rows), bf16),
            shape((rows, D), bf16),
            shape((rows, D), bf16),
            shape((rows, 3 * D), f32),
            shape((8, D), f32),
            shape((rows, D), f32),
            shape((rows, FF), bf16),
            shape((rows, 2 * FF), bf16),
            shape((rows, D), f32),
            shape((rows, D), bf16),
            shape((n_heads, D, HEAD), bf16),
            shape((8, D), bf16),
        ),
        in_specs=[
            pl.BlockSpec(memory_space=pltpu.SMEM),
            anywhere,
            anywhere,
            anywhere,
            vmem,
            vmem,
        ],
        out_specs=(anywhere,) * 12,
        scratch_shapes=[
            pltpu.VMEM(tokens.shape, bf16),
            pltpu.VMEM(tokens.shape, bf16),
            pltpu.VMEM((n_heads, D, HEAD), bf16),
            pltpu.VMEM((n_trios, D, 3 * TRIO), bf16),
            pltpu.VMEM((8, D), bf16),
            pltpu.VMEM((rows, D), bf16),
            pltpu.VMEM((rows, D), bf16),
            pltpu.VMEM((rows, D), bf16),
            pltpu.VMEM((rows, D), bf16),
            pltpu.VMEM((rows, D), bf16),
            pltpu.VMEM((D, rows), bf16),
            pltpu.VMEM((rows, 3 * D), f32),
            pltpu.VMEM((8, D), f32),
            pltpu.VMEM((rows, D), f32),
            pltpu.VMEM((rows + 8, D), f32),
            pltpu.VMEM((2, rows, TRIO), bf16),
            pltpu.VMEM((2, rows, 2 * TRIO), bf16),
            pltpu.SemaphoreType.DMA((3,)),
            pltpu.SemaphoreType.DMA((n_heads + 3 * n_trios,)),
            pltpu.SemaphoreType.DMA((2, 7)),
            pltpu.SemaphoreType.DMA((2, 7)),
            pltpu.SemaphoreType.DMA((3,)),
            pltpu.SemaphoreType.DMA((3,)),
            pltpu.SemaphoreType.DMA((6, count)),
            pltpu.SemaphoreType.DMA((6, count)),
            pltpu.SemaphoreType.DMA((2,)),
            pltpu.SemaphoreType.DMA((10,)),
            pltpu.SemaphoreType.DMA((2, 3)),
        ],
        compiler_params=pltpu.CompilerParams(
            collective_id=1, has_side_effects=True, vmem_limit_bytes=63 << 20
        ),
        cost_estimate=pl.CostEstimate(
            flops=8 * rows * D * FF, bytes_accessed=10**8, transcendentals=0
        ),
        name="gathered_forward",
    )(deal_order, tokens, dys, weights, small, masks)


def contract_units(left, units):
    return sum(
        contract_cols(left[:, u * HEAD : (u + 1) * HEAD], units[u]) for u in range(units.shape[0])
    )


def shards(
    tokens_in,
    out_grad,
    deal_order,
    seq_lengths,
    weights,
    norm_gains,
    conv_kernel,
    vector_state,
    kron_stats,
    kron_roots,
):
    n_seq = lax.axis_size("seq")
    n_wsh = lax.axis_size("wsh")
    rows = tokens_in.shape[1]
    unit = rows // n_seq
    first_row = lax.axis_index("seq") * rows
    pos = seq_positions(seq_lengths[0], first_row, rows + 2)
    masks = [(pos >= 2 - k).astype(jnp.float32)[:, None] for k in range(3)]
    small = jnp.concatenate(
        [norm_gains, conv_kernel, jnp.zeros((3, norm_gains.shape[1]), jnp.bfloat16)], axis=0
    )
    (
        lefts,
        x_bf,
        dy_bf,
        proj,
        prev,
        hidden_sum,
        act,
        d_gu,
        d_hn,
        result,
        heads,
        smalls,
    ) = gathered_forward(
        deal_order,
        tokens_in.reshape(n_seq, unit, D),
        out_grad.reshape(n_seq, unit, D),
        weights,
        small,
        jnp.stack([masks[0][:rows], masks[1][:rows]]),
    )
    gains = smalls[:2].astype(jnp.float32)
    kernel = smalls[2:5].astype(jnp.float32)
    xf = x_bf.astype(jnp.float32)
    scale_one = rms_scale(xf)
    scale_two = rms_scale(hidden_sum)
    b_part = proj[:, :D]
    c_part = proj[:, D : 2 * D]
    x_part = proj[:, 2 * D :]
    ext = jnp.concatenate([prev[6:], b_part * x_part], axis=0)
    conv = (
        kernel[0] * masks[0][:rows] * ext[0:rows]
        + kernel[1] * masks[1][:rows] * ext[1 : rows + 1]
        + kernel[2] * masks[2][:rows] * ext[2 : rows + 2]
    )
    d_norm_two, g_gain_two = norm_back(d_hn, hidden_sum, scale_two, gains[1])
    d_hidden = dy_bf.astype(jnp.float32) + d_norm_two
    d_mix = d_hidden.astype(jnp.bfloat16)
    d_yc = contract_units(d_mix, heads[3 * D // HEAD :])
    d_c = d_yc * conv
    d_conv = d_yc * c_part
    after = passed_along(d_conv[:2], "seq", -1)
    d_ext = jnp.concatenate([d_conv, after], axis=0)
    weighted = [d_ext * masks[k] for k in range(3)]
    d_bx = (
        kernel[2] * weighted[2][:rows]
        + kernel[1] * weighted[1][1 : rows + 1]
        + kernel[0] * weighted[0][2 : rows + 2]
    )
    g_taps = jnp.stack([jnp.sum(weighted[k][:rows] * ext[k : k + rows], axis=0) for k in range(3)])
    d_proj = jnp.concatenate([d_bx * x_part, d_c, d_bx * b_part], axis=1).astype(jnp.bfloat16)
    d_xn = contract_units(d_proj, heads[: 3 * D // HEAD])
    d_norm_one, g_gain_one = norm_back(d_xn, xf, scale_one, gains[0])
    d_input = (d_hidden + d_norm_one).astype(jnp.bfloat16)
    g_vec = jnp.concatenate([g_gain_one[None], g_gain_two[None], g_taps], axis=0)
    inverse = jnp.argsort(deal_order)
    result_leaving = jnp.take(result.reshape(n_seq, unit, D), inverse, axis=0)
    result_back = lax.all_to_all(result_leaving, "seq", split_axis=0, concat_axis=0, tiled=True)
    leaving = jnp.take(d_input.reshape(n_seq, unit, D), inverse, axis=0)
    ncol_blocks = weights.shape[1] // BLK
    nrow_blocks = weights.shape[0] // BLK
    share = BLK // n_seq
    roots_r = lax.all_gather(kron_roots[1].astype(jnp.bfloat16), "seq", axis=1, tiled=True)
    vec = jnp.pad(g_vec.T.astype(jnp.bfloat16), ((0, 0), (0, COLS - g_vec.shape[0])))
    grad_bf, terms, dx_back = reduced(
        lefts,
        (d_proj, d_mix, d_gu, act),
        vec.reshape(n_wsh, D // n_wsh, COLS),
        kron_roots[0].astype(jnp.bfloat16).reshape(nrow_blocks, ncol_blocks, share, BLK),
        roots_r.reshape(nrow_blocks, ncol_blocks, BLK, BLK),
        leaving,
        float((rows * n_seq * n_wsh) ** -0.5),
    )
    grad_shard = grad_bf[:, : weights.shape[1]].astype(jnp.float32)
    vec_grad = grad_bf[:, weights.shape[1] : weights.shape[1] + 5].astype(jnp.float32).T
    state_new = BETA_VEC * vector_state + (1.0 - BETA_VEC) * vec_grad * vec_grad
    vec_update = -LEARN_VEC * vec_grad * lax.rsqrt(state_new)
    terms = terms.reshape(3, nrow_blocks * ncol_blocks, share, BLK).astype(jnp.float32)
    stats_new = BETA * kron_stats + ((1.0 - BETA) / BLK) * terms[:2]
    return (
        result_back.reshape(1, rows, D),
        dx_back.reshape(1, rows, D),
        grad_shard,
        vec_grad,
        state_new,
        vec_update,
        stats_new,
        -LEARN * terms[2],
    )


def solution(mesh):
    known = mesh.shape["seq"] == 8 and mesh.shape["wsh"] == 4
    return jax.shard_map(
        shards if known else plain_shards,
        mesh=mesh,
        in_specs=(
            P("wsh", "seq", None),
            P("wsh", "seq", None),
            P(),
            P("wsh", None),
            P("wsh", None),
            P(None, "wsh"),
            P(None, "wsh"),
            P(None, "wsh"),
            P(None, "wsh", "seq", None),
            P(None, "wsh", "seq", None),
        ),
        out_specs=(
            P("wsh", "seq", None),
            P("wsh", "seq", None),
            P("wsh", None),
            P(None, "wsh"),
            P(None, "wsh"),
            P(None, "wsh"),
            P(None, "wsh", "seq", None),
            P("wsh", "seq", None),
        ),
        check_vma=False,
    )
```

```python
import functools

import jax
import jax.numpy as jnp
from jax import lax
from jax.experimental import pallas as pl
from jax.experimental.pallas import tpu as pltpu
from jax.sharding import PartitionSpec as P

MESH = pl.DeviceIdType.MESH

D = 1024
FF = 4608
BLK = 128


EPS = 1e-05
BETA = 0.5
BETA_VEC = 0.5
LEARN = 0.03
LEARN_VEC = 0.05
HIGH = lax.Precision.HIGHEST


def passed_along(block, axis, distance):
    devices = range(lax.axis_size(axis))
    route = [(i - distance, i) for i in devices if i - distance in devices]
    return lax.ppermute(block, axis, route)


def seq_positions(lengths_row, first, count):
    starts = jnp.cumsum(lengths_row) - lengths_row
    rows_at = first + jnp.arange(count, dtype=jnp.int32)
    begin = jnp.max(jnp.where(starts[None, :] <= rows_at[:, None], starts[None, :], 0), axis=1)
    return rows_at - begin


def rms_scale(values):
    return lax.rsqrt(jnp.mean(values * values, axis=1, keepdims=True) + EPS)


def norm_back(upstream, values, scale, gain):
    scaled = upstream * gain
    inner = jnp.mean(scaled * values, axis=1, keepdims=True)
    return (
        scale * scaled - values * scale * scale * scale * inner,
        jnp.sum(upstream * values * scale, axis=0),
    )


def contract_rows(left, right):
    return lax.dot_general(
        left, right, (((0,), (0,)), ((), ())), preferred_element_type=jnp.float32
    )


def contract_cols(left, right):
    return lax.dot_general(
        left, right, (((1,), (1,)), ((), ())), preferred_element_type=jnp.float32
    )


def plain_shards(
    tokens_in,
    out_grad,
    deal_order,
    seq_lengths,
    weights,
    norm_gains,
    conv_kernel,
    vector_state,
    kron_stats,
    kron_roots,
):
    n_seq = lax.axis_size("seq")
    n_wsh = lax.axis_size("wsh")
    rows = tokens_in.shape[1]
    unit = rows // n_seq
    arrived = (
        lax.all_to_all(
            tokens_in.reshape(n_seq, unit, D), "seq", split_axis=0, concat_axis=0, tiled=True
        ),
        lax.all_to_all(
            out_grad.reshape(n_seq, unit, D), "seq", split_axis=0, concat_axis=0, tiled=True
        ),
    )
    x_bf = jnp.take(arrived[0], deal_order, axis=0).reshape(rows, D)
    dy_bf = jnp.take(arrived[1], deal_order, axis=0).reshape(rows, D)
    full_w, gains_bf, kernel_bf = (
        lax.all_gather(weights, "wsh", axis=0, tiled=True),
        lax.all_gather(norm_gains, "wsh", axis=1, tiled=True),
        lax.all_gather(conv_kernel, "wsh", axis=1, tiled=True),
    )
    gains = gains_bf.astype(jnp.float32)
    kernel = kernel_bf.astype(jnp.float32)
    first_row = lax.axis_index("seq") * rows
    pos = seq_positions(seq_lengths[0], first_row, rows + 2)
    masks = [(pos >= 2 - k).astype(jnp.float32)[:, None] for k in range(3)]
    xf = x_bf.astype(jnp.float32)
    scale_one = rms_scale(xf)
    xn = (xf * scale_one * gains[0]).astype(jnp.bfloat16)
    proj = jnp.dot(xn, full_w[:, : 3 * D], preferred_element_type=jnp.float32)
    b_part = proj[:, :D]
    c_part = proj[:, D : 2 * D]
    x_part = proj[:, 2 * D :]
    conv_in = b_part * x_part
    prev = passed_along(conv_in[rows - 2 :], "seq", 1)
    ext = jnp.concatenate([prev, conv_in], axis=0)
    conv = (
        kernel[0] * masks[0][:rows] * ext[0:rows]
        + kernel[1] * masks[1][:rows] * ext[1 : rows + 1]
        + kernel[2] * masks[2][:rows] * ext[2 : rows + 2]
    )
    yc = (c_part * conv).astype(jnp.bfloat16)
    hidden_sum = xf + jnp.dot(yc, full_w[:, 3 * D : 4 * D], preferred_element_type=jnp.float32)
    scale_two = rms_scale(hidden_sum)
    hn = (hidden_sum * scale_two * gains[1]).astype(jnp.bfloat16)
    gate_up = jnp.dot(hn, full_w[:, 4 * D : 4 * D + 2 * FF], preferred_element_type=jnp.float32)
    gate = gate_up[:, :FF]
    upper = gate_up[:, FF:]
    sig = jax.nn.sigmoid(gate)
    act = (gate * sig * upper).astype(jnp.bfloat16)
    ffn = contract_cols(act, full_w[:, 4 * D + 2 * FF :])
    result = (hidden_sum + ffn).astype(jnp.bfloat16)
    g_down = contract_rows(dy_bf, act)
    d_act = jnp.dot(dy_bf, full_w[:, 4 * D + 2 * FF :], preferred_element_type=jnp.float32)
    d_gate = d_act * upper * sig * (1.0 + gate * (1.0 - sig))
    d_upper = d_act * gate * sig
    d_gu = jnp.concatenate([d_gate, d_upper], axis=1).astype(jnp.bfloat16)
    g_gu = contract_rows(hn, d_gu)
    d_hn = contract_cols(d_gu, full_w[:, 4 * D : 4 * D + 2 * FF])
    d_norm_two, g_gain_two = norm_back(d_hn, hidden_sum, scale_two, gains[1])
    d_hidden = dy_bf.astype(jnp.float32) + d_norm_two
    d_mix = d_hidden.astype(jnp.bfloat16)
    g_out = contract_rows(yc, d_mix)
    d_yc = contract_cols(d_mix, full_w[:, 3 * D : 4 * D])
    d_c = d_yc * conv
    d_conv = d_yc * c_part
    after = passed_along(d_conv[:2], "seq", -1)
    d_ext = jnp.concatenate([d_conv, after], axis=0)
    weighted = [d_ext * masks[k] for k in range(3)]
    d_bx = (
        kernel[2] * weighted[2][:rows]
        + kernel[1] * weighted[1][1 : rows + 1]
        + kernel[0] * weighted[0][2 : rows + 2]
    )
    g_taps = jnp.stack([jnp.sum(weighted[k][:rows] * ext[k : k + rows], axis=0) for k in range(3)])
    d_proj = jnp.concatenate([d_bx * x_part, d_c, d_bx * b_part], axis=1).astype(jnp.bfloat16)
    g_in = contract_rows(xn, d_proj)
    d_xn = contract_cols(d_proj, full_w[:, : 3 * D])
    d_norm_one, g_gain_one = norm_back(d_xn, xf, scale_one, gains[0])
    d_input = (d_hidden + d_norm_one).astype(jnp.bfloat16)
    g_vec = jnp.concatenate([g_gain_one[None], g_gain_two[None], g_taps], axis=0)
    inverse = jnp.argsort(deal_order)
    leaving = (
        jnp.take(result.reshape(n_seq, unit, D), inverse, axis=0),
        jnp.take(d_input.reshape(n_seq, unit, D), inverse, axis=0),
    )
    returned = (
        lax.all_to_all(leaving[0], "seq", split_axis=0, concat_axis=0, tiled=True),
        lax.all_to_all(leaving[1], "seq", split_axis=0, concat_axis=0, tiled=True),
    )
    summed = (
        lax.psum_scatter(g_in.astype(jnp.bfloat16), "wsh", scatter_dimension=0, tiled=True).astype(
            jnp.float32
        ),
        lax.psum_scatter(g_out.astype(jnp.bfloat16), "wsh", scatter_dimension=0, tiled=True).astype(
            jnp.float32
        ),
        lax.psum_scatter(g_gu.astype(jnp.bfloat16), "wsh", scatter_dimension=0, tiled=True).astype(
            jnp.float32
        ),
        lax.psum_scatter(
            g_down.astype(jnp.bfloat16), "wsh", scatter_dimension=0, tiled=True
        ).astype(jnp.float32),
        lax.psum_scatter(g_vec.astype(jnp.bfloat16), "wsh", scatter_dimension=1, tiled=True).astype(
            jnp.float32
        ),
    )
    summed = (
        lax.psum(summed[0].astype(jnp.bfloat16), "seq").astype(jnp.float32),
        lax.psum(summed[1].astype(jnp.bfloat16), "seq").astype(jnp.float32),
        lax.psum(summed[2].astype(jnp.bfloat16), "seq").astype(jnp.float32),
        lax.psum(summed[3].astype(jnp.bfloat16), "seq").astype(jnp.float32),
        lax.psum(summed[4].astype(jnp.bfloat16), "seq").astype(jnp.float32),
    )
    grad_scale = lax.rsqrt(jnp.asarray(rows * n_seq * n_wsh, jnp.float32))
    grad_shard = jnp.concatenate([summed[0], summed[1], summed[2], summed[3]], axis=1) * grad_scale
    vec_grad = summed[4] * grad_scale
    state_new = BETA_VEC * vector_state + (1.0 - BETA_VEC) * vec_grad * vec_grad
    vec_update = -LEARN_VEC * vec_grad * lax.rsqrt(state_new)
    nrow_blocks = grad_shard.shape[0] // BLK
    ncol_blocks = grad_shard.shape[1] // BLK
    grad_blocks = (
        grad_shard.reshape(nrow_blocks, BLK, ncol_blocks, BLK)
        .transpose(0, 2, 1, 3)
        .reshape(nrow_blocks * ncol_blocks, BLK, BLK)
    )
    share = BLK // n_seq
    first_block_row = lax.axis_index("seq") * share
    block_rows = lax.dynamic_slice_in_dim(grad_blocks, first_block_row, share, 1)
    block_cols = lax.dynamic_slice_in_dim(grad_blocks, first_block_row, share, 2)
    left_term = jnp.einsum("nij,nkj->nik", block_rows, grad_blocks, precision=HIGH)
    right_term = jnp.einsum("nji,njk->nik", block_cols, grad_blocks, precision=HIGH)
    stats_new = jnp.stack(
        [
            BETA * kron_stats[0] + (1.0 - BETA) * left_term / BLK,
            BETA * kron_stats[1] + (1.0 - BETA) * right_term / BLK,
        ]
    )
    right_full = lax.all_gather(
        kron_roots[1].astype(jnp.bfloat16), "seq", axis=1, tiled=True
    ).astype(jnp.float32)
    left_mul = jnp.einsum("nij,njk->nik", kron_roots[0], grad_blocks, precision=HIGH)
    update = -LEARN * jnp.einsum("nij,njk->nik", left_mul, right_full, precision=HIGH)
    return (
        returned[0].reshape(1, rows, D),
        returned[1].reshape(1, rows, D),
        grad_shard,
        vec_grad,
        state_new,
        vec_update,
        stats_new,
        update,
    )


COLS = 256
GAP = 2
RING = 14
SEMS = 4
BATCHES = 5


def place():
    seq, wsh = lax.axis_index("seq"), lax.axis_index("wsh")
    return seq // 2, seq % 2, wsh // 2, wsh % 2


def reduce_kernel(
    edges,
    scale,
    lefts_ref,
    d_in_ref,
    d_mix_ref,
    d_gu_ref,
    act_ref,
    vec_ref,
    owned_ref,
    leave_ref,
    leave_two_ref,
    grad_ref,
    terms_ref,
    update_ref,
    arrive_ref,
    arrive_two_ref,
    b_buf,
    g_buf,
    core_in,
    y_out,
    y_in,
    x_out,
    x_in,
    pair_out,
    pair_in,
    far_out,
    far_in,
    final,
    r_buf,
    t_buf,
    u_buf,
    b_sem,
    r_sem,
    o_sem,
    t_sem,
    send_sem,
    recv_sem,
    far_send,
    far_recv,
    own_sem,
    back_send,
    back_recv,
):
    z, x, y, c = place()
    seq, wsh = lax.axis_index("seq"), lax.axis_index("wsh")
    n_real = edges[-1]
    count = n_real + 1
    core_id = (seq, y * 2 + (1 - c))
    y_id = (seq, (1 - y) * 2 + c)
    x_id = (z * 2 + (1 - x), wsh)
    high, low = z // 2, z % 2
    pair_id = ((2 * high + 1 - low) * 2 + x, wsh)
    over_id = ((2 * (1 - high) + low) * 2 + x, wsh)
    owned_row = x * 128 + low * 64 + high * 32
    far_ids = [(lax.rem(seq + d, 8), wsh) for d in range(1, 8)]

    barrier = pltpu.get_barrier_semaphore()
    for device in [core_id, y_id] + far_ids:
        pl.semaphore_signal(barrier, inc=1, device_id=device, device_id_type=MESH)
    pl.semaphore_wait(barrier, 9)

    def far(k, d):
        source, target = ((leave_ref, arrive_ref), (leave_two_ref, arrive_two_ref))[k]
        to = far_ids[d - 1]
        return pltpu.make_async_remote_copy(
            src_ref=source.at[to[0]],
            dst_ref=target.at[seq],
            send_sem=far_send.at[k, d - 1],
            recv_sem=far_recv.at[k, d - 1],
            device_id=to,
            device_id_type=MESH,
        )

    own_pairs = ((leave_ref, arrive_ref), (leave_two_ref, arrive_two_ref))
    for k, (source, target) in enumerate(own_pairs):
        pltpu.make_async_copy(source.at[seq], target.at[seq], own_sem.at[k]).start()
        for d in range(1, 8):
            far(k, d).start()

    batch = update_ref.shape[1] // BATCHES

    def u_piece(ref, device, b):
        return ref.at[device, pl.ds(b * batch, batch)]

    def u_back(b, d):
        to = far_ids[d - 1]
        return pltpu.make_async_remote_copy(
            src_ref=u_piece(u_buf, to[0], b),
            dst_ref=u_piece(update_ref, seq, b),
            send_sem=back_send.at[b, d - 1],
            recv_sem=back_recv.at[b, d - 1],
            device_id=to,
            device_id_type=MESH,
        )

    def u_own(b):
        return pltpu.make_async_copy(
            u_piece(u_buf, seq, b), u_piece(update_ref, seq, b), own_sem.at[2 + b]
        )

    def remote(flow, n, source, target, device):
        k = lax.rem(n, SEMS)
        return pltpu.make_async_remote_copy(
            src_ref=source,
            dst_ref=target,
            send_sem=send_sem.at[flow, k],
            recv_sem=recv_sem.at[flow, k],
            device_id=device,
            device_id_type=MESH,
        )

    def core_copy(n):
        slot = lax.rem(n, RING)
        return remote(0, n, g_buf.at[slot, 1 - c], core_in.at[slot], core_id)

    def y_copy(n):
        return remote(1, n, y_out.at[lax.rem(n, SEMS)], y_in.at[lax.rem(n, RING)], y_id)

    def x_copy(n):
        return remote(2, n, x_out.at[lax.rem(n, SEMS)], x_in.at[lax.rem(n, RING)], x_id)

    def pair_copy(n):
        return remote(
            3, n, pair_out.at[lax.rem(n, SEMS)], pair_in.at[lax.rem(n, RING)], pair_id
        )

    def over_copy(n):
        return remote(4, n, far_out.at[lax.rem(n, SEMS)], far_in.at[lax.rem(n, RING)], over_id)

    def final_rows(n, first, size):
        return final.at[lax.rem(n, RING), pl.ds(pl.multiple_of(first, size), size)]

    def over_share(n):
        piece = final_rows(n, owned_row, 32)
        return remote(5, n, piece, piece, over_id)

    def pair_share(n):
        piece = final_rows(n, x * 128 + low * 64, 64)
        return remote(6, n, piece, piece, pair_id)

    def x_share(n):
        piece = final_rows(n, x * 128, 128)
        return remote(7, n, piece, piece, x_id)

    def b_copies(n):
        slot = lax.rem(n, SEMS)
        column = n_real - n
        for r, source in enumerate((d_in_ref, d_mix_ref, d_gu_ref, act_ref)):
            low, high = edges[r], edges[r + 1]
            at = jnp.clip(column - low, 0, high - low - 1)
            at = pl.multiple_of(at * COLS, COLS)
            copy = pltpu.make_async_copy(
                source.at[:, pl.ds(at, COLS)], b_buf.at[slot], b_sem.at[slot]
            )
            yield (column >= low) & (column < high), copy

    def r_copies(n):
        slot = lax.rem(n, SEMS)
        at = jnp.minimum(n_real - n, n_real - 1) // 2
        return [
            pltpu.make_async_copy(
                owned_ref.at[:, kind, at], r_buf.at[slot, kind], r_sem.at[slot, kind]
            )
            for kind in range(2)
        ]

    def has_block(n):
        return (n > 0) & (lax.rem(n_real - n, 2) == lax.rem(seq, 4) // 2)

    def o_copy(n):
        at = pl.multiple_of((n_real - n) * COLS, COLS)
        return pltpu.make_async_copy(
            final.at[lax.rem(n, RING)], grad_ref.at[:, pl.ds(at, COLS)], o_sem.at[lax.rem(n, SEMS)]
        )

    def t_copy(n):
        slot = lax.rem(n, SEMS)
        at = pl.multiple_of(jnp.minimum(n_real - n, n_real - 1) * 2, 2)
        return pltpu.make_async_copy(
            t_buf.at[slot], terms_ref.at[:, :, pl.ds(at, 2)], t_sem.at[slot]
        )

    def wide(value):
        return value.astype(jnp.float32)

    def sum_rows(slot, first, size):
        rows = pl.ds(pl.multiple_of(first, size), size)
        total = wide(g_buf[slot, c, y, rows]) + wide(core_in[slot, y, rows])
        return total + wide(y_in[slot, rows])

    def sum_half(slot, row, size):
        rows = pl.ds(pl.multiple_of(row, size), size)
        return sum_rows(slot, x * 128 + row, size) + wide(x_in[slot, rows])

    def stage_load(n):
        for wanted, copy in b_copies(n):
            pl.when(wanted)(copy.start)

    def stage_product(n):
        slot = lax.rem(n, RING)
        column = n_real - n

        @pl.when(n > 0)
        def _():
            for wanted, copy in b_copies(n):
                pl.when(wanted)(copy.wait)
            region = sum((column >= e).astype(jnp.int32) for e in edges[1:-1])
            right = b_buf[lax.rem(n, SEMS)]
            for w in range(4):
                product = jnp.dot(
                    lefts_ref[region, w * 256 : (w + 1) * 256, :],
                    right,
                    preferred_element_type=jnp.float32,
                )
                g_buf[slot, w % 2, w // 2] = product.astype(jnp.bfloat16)

        @pl.when(n == 0)
        def _():
            for w in range(4):
                g_buf[slot, w % 2, w // 2] = vec_ref[w]

        core_copy(n).start()

    def stage_y(n):
        slot = lax.rem(n, RING)
        core_copy(n).wait()
        y_out[lax.rem(n, SEMS)] = (
            wide(g_buf[slot, c, 1 - y]) + wide(core_in[slot, 1 - y])
        ).astype(jnp.bfloat16)
        y_copy(n).start()

    def stage_x(n):
        slot = lax.rem(n, RING)
        y_copy(n).wait()
        x_out[lax.rem(n, SEMS)] = sum_rows(slot, (1 - x) * 128, 128).astype(jnp.bfloat16)
        x_copy(n).start()

    def stage_pair(n):
        slot = lax.rem(n, RING)
        x_copy(n).wait()
        total = sum_half(slot, (1 - low) * 64, 64)
        pair_out[lax.rem(n, SEMS)] = total.astype(jnp.bfloat16)
        pair_copy(n).start()

    def stage_over(n):
        slot = lax.rem(n, RING)
        pair_copy(n).wait()
        row = (1 - high) * 32
        total = sum_half(slot, low * 64 + row, 32)
        total = total + wide(pair_in[slot, pl.ds(pl.multiple_of(row, 32), 32)])
        far_out[lax.rem(n, SEMS)] = total.astype(jnp.bfloat16)
        over_copy(n).start()

    def stage_final(n):
        slot = lax.rem(n, RING)
        over_copy(n).wait()
        total = sum_half(slot, low * 64 + high * 32, 32)
        total = total + wide(pair_in[slot, pl.ds(pl.multiple_of(high * 32, 32), 32)])
        total = total + wide(far_in[slot])
        final[slot, pl.ds(pl.multiple_of(owned_row, 32), 32)] = (total * scale).astype(
            jnp.bfloat16
        )
        over_share(n).start()

    def stage_pair_share(n):
        over_share(n).wait()
        pair_share(n).start()

    def stage_share(n):
        pair_share(n).wait()
        x_share(n).start()

        @pl.when(has_block(n))
        def _():
            for copy in r_copies(n):
                copy.start()


    def stage_take(n):
        x_share(n).wait()
        o_copy(n).start()

    def stage_use(n):
        slot = lax.rem(n, RING)
        part = lax.rem(n, SEMS)

        @pl.when(n > SEMS)
        def _():
            t_copy(n - SEMS).wait()

        @pl.when(n > 0)
        def _():
            picked = lax.broadcasted_iota(jnp.int32, (16, BLK), 1) == (
                lax.broadcasted_iota(jnp.int32, (16, BLK), 0) + seq * 16
            )
            one_hot = picked.astype(jnp.float32).astype(jnp.bfloat16)
            for i in range(2):
                for j in range(2):
                    lanes = slice(j * BLK, (j + 1) * BLK)
                    block = final[slot, i * BLK : (i + 1) * BLK, lanes]
                    rows = final[
                        slot, pl.ds(pl.multiple_of(i * BLK + seq * 16, 16), 16), lanes
                    ]
                    first = contract_cols(jnp.concatenate([rows, one_hot], axis=0), block)
                    second = jnp.dot(
                        first[16:].astype(jnp.bfloat16),
                        block,
                        preferred_element_type=jnp.float32,
                    )
                    t_buf[part, 0, i, j] = first[:16].astype(jnp.bfloat16)
                    t_buf[part, 1, i, j] = second.astype(jnp.bfloat16)
            t_copy(n).start()

        @pl.when(has_block(n))
        def _():
            for copy in r_copies(n):
                copy.wait()
            block = final[
                slot,
                pl.ds(pl.multiple_of(seq // 4 * BLK, BLK), BLK),
                pl.ds(pl.multiple_of(lax.rem(seq, 2) * BLK, BLK), BLK),
            ]
            left = jnp.dot(
                r_buf[part, 0].reshape(BLK, BLK), block, preferred_element_type=jnp.float32
            )
            both = jnp.dot(
                left.astype(jnp.bfloat16),
                r_buf[part, 1].reshape(BLK, BLK),
                preferred_element_type=jnp.float32,
            )
            u_buf[:, (n_real - n) // 2] = both.astype(jnp.bfloat16).reshape(8, 16, BLK)

        column = n_real - n

        @pl.when((n > 0) & (lax.rem(column, 2 * batch) == 0))
        def _():
            b = column // (2 * batch)
            u_own(b).start()
            for d in range(1, 8):
                u_back(b, d).start()

    def stage_done(n):
        o_copy(n).wait()

    offsets = {
        "load": 0,
        "product": GAP,
        "y": 2 * GAP,
        "x": 3 * GAP,
        "pair": 4 * GAP,
        "over": 5 * GAP,
        "final": 6 * GAP,
        "pair_share": 7 * GAP,
        "share": 8 * GAP,
        "take": 9 * GAP,
        "use": 9 * GAP,
        "done": 10 * GAP,
    }
    stages = (
        ("done", stage_done),
        ("take", stage_take),
        ("share", stage_share),
        ("pair_share", stage_pair_share),
        ("final", stage_final),
        ("over", stage_over),
        ("pair", stage_pair),
        ("x", stage_x),
        ("y", stage_y),
        ("product", stage_product),
        ("load", stage_load),
        ("use", stage_use),
    )

    def step(t, carry):
        for name, stage in stages:
            n = t - offsets[name]
            pl.when((n >= 0) & (n < count))(functools.partial(stage, n))
        return carry

    lax.fori_loop(0, count + offsets["done"], step, 0)
    for n in range(count - SEMS, count):
        t_copy(n).wait()
    for k, (source, target) in enumerate(own_pairs):
        pltpu.make_async_copy(source.at[seq], target.at[seq], own_sem.at[k]).wait()
        for d in range(1, 8):
            far(k, d).wait()
    for b in range(BATCHES):
        u_own(b).wait()
        for d in range(1, 8):
            u_back(b, d).wait()


def reduced(lefts, rights, vec, owned, leaving, scale):
    edges = [0]
    for right in rights:
        edges.append(edges[-1] + right.shape[1] // COLS)
    rows = rights[0].shape[0]
    count = edges[-1]
    bf16 = jnp.bfloat16
    anywhere = pl.BlockSpec(memory_space=pl.ANY)
    vmem = pl.BlockSpec(memory_space=pltpu.VMEM)
    return pl.pallas_call(
        functools.partial(reduce_kernel, tuple(edges), scale),
        out_shape=(
            jax.ShapeDtypeStruct((256, (count + 1) * COLS), bf16),
            jax.ShapeDtypeStruct((2, 2, count * 2, 16, BLK), bf16),
            jax.ShapeDtypeStruct((8, count // 2, 16, BLK), bf16),
            jax.ShapeDtypeStruct(leaving[0].shape, bf16),
            jax.ShapeDtypeStruct(leaving[1].shape, bf16),
        ),
        in_specs=[vmem, anywhere, anywhere, anywhere, anywhere, vmem, anywhere, anywhere, anywhere],
        out_specs=(anywhere,) * 5,
        scratch_shapes=[
            pltpu.VMEM((SEMS, rows, COLS), bf16),
            pltpu.VMEM((RING, 2, 2, 256, COLS), bf16),
            pltpu.VMEM((RING, 2, 256, COLS), bf16),
            pltpu.VMEM((SEMS, 256, COLS), bf16),
            pltpu.VMEM((RING, 256, COLS), bf16),
            pltpu.VMEM((SEMS, 128, COLS), bf16),
            pltpu.VMEM((RING, 128, COLS), bf16),
            pltpu.VMEM((SEMS, 64, COLS), bf16),
            pltpu.VMEM((RING, 64, COLS), bf16),
            pltpu.VMEM((SEMS, 32, COLS), bf16),
            pltpu.VMEM((RING, 32, COLS), bf16),
            pltpu.VMEM((RING, 256, COLS), bf16),
            pltpu.VMEM((SEMS, 2, 8, 16, BLK), bf16),
            pltpu.VMEM((SEMS, 2, 2, 2, 16, BLK), bf16),
            pltpu.VMEM((8, count // 2, 16, BLK), bf16),
            pltpu.SemaphoreType.DMA((SEMS,)),
            pltpu.SemaphoreType.DMA((SEMS, 2)),
            pltpu.SemaphoreType.DMA((SEMS,)),
            pltpu.SemaphoreType.DMA((SEMS,)),
            pltpu.SemaphoreType.DMA((8, SEMS)),
            pltpu.SemaphoreType.DMA((8, SEMS)),
            pltpu.SemaphoreType.DMA((2, 7)),
            pltpu.SemaphoreType.DMA((2, 7)),
            pltpu.SemaphoreType.DMA((2 + BATCHES,)),
            pltpu.SemaphoreType.DMA((BATCHES, 7)),
            pltpu.SemaphoreType.DMA((BATCHES, 7)),
        ],
        compiler_params=pltpu.CompilerParams(
            collective_id=0, has_side_effects=True, vmem_limit_bytes=48 << 20
        ),
        cost_estimate=pl.CostEstimate(
            flops=2 * rows * 1024 * count * COLS, bytes_accessed=10**9, transcendentals=0
        ),
        name="reduce_chunks",
    )(lefts, *rights, vec, owned, *leaving)


HEAD = 512
TRIO = 256


def forward_kernel(
    deal_ref,
    tokens_ref,
    dy_ref,
    weights_ref,
    small_ref,
    masks_ref,
    roots_ref,
    lefts_ref,
    x_ref,
    dy_out_ref,
    proj_ref,
    prev_ref,
    h_ref,
    act_ref,
    d_gu_ref,
    d_hn_ref,
    result_ref,
    heads_ref,
    smalls_ref,
    owned_ref,
    x_in,
    dy_in,
    heads,
    trios,
    smalls,
    xs,
    dys,
    xn,
    yc,
    hn,
    turned,
    proj,
    mixed,
    total,
    back,
    act_buf,
    d_gu_buf,
    own_sem,
    load_sem,
    far_send,
    far_recv,
    small_send,
    small_recv,
    send_sem,
    recv_sem,
    halo_sem,
    out_sem,
    act_sem,
):
    z, x, y, c = place()
    seq, wsh = lax.axis_index("seq"), lax.axis_index("wsh")
    bf16 = jnp.bfloat16
    n_heads, n_trios = heads.shape[0], trios.shape[0]
    count = n_heads + n_trios
    core_id = (seq, y * 2 + (1 - c))
    y_id = (seq, (1 - y) * 2 + c)
    cross_id = (seq, (1 - y) * 2 + (1 - c))
    x_id = (z * 2 + (1 - x), wsh)
    z_id = ((z + 1 - 2 * (z % 2)) * 2 + x, wsh)
    far_ids = [(lax.rem(seq + d, 8), wsh) for d in range(1, 8)]
    quarter = x * 2 + z % 2
    mine = pl.multiple_of(wsh * 256, 256)
    theirs = pl.multiple_of(((1 - y) * 2 + c) * 256, 256)

    barrier = pltpu.get_barrier_semaphore()
    for device in [core_id, y_id, cross_id] + far_ids:
        pl.semaphore_signal(barrier, inc=1, device_id=device, device_id_type=MESH)
    pl.semaphore_wait(barrier, 10)

    def far(k, d, source, target):
        to = lax.rem(seq + d, 8)
        return pltpu.make_async_remote_copy(
            src_ref=source.at[to],
            dst_ref=target.at[seq],
            send_sem=far_send.at[k, d - 1],
            recv_sem=far_recv.at[k, d - 1],
            device_id=(to, wsh),
            device_id_type=MESH,
        )

    def small_copy(k, to):
        return pltpu.make_async_remote_copy(
            src_ref=small_ref,
            dst_ref=smalls.at[:, pl.ds(mine, 256)],
            send_sem=small_send.at[k],
            recv_sem=small_recv.at[k],
            device_id=to,
            device_id_type=MESH,
        )

    small_ids = (core_id, y_id, cross_id)
    own_copies = (
        pltpu.make_async_copy(tokens_ref.at[seq], x_in.at[seq], own_sem.at[0]),
        pltpu.make_async_copy(dy_ref.at[seq], dy_in.at[seq], own_sem.at[1]),
        pltpu.make_async_copy(small_ref, smalls.at[:, pl.ds(mine, 256)], own_sem.at[2]),
        pltpu.make_async_copy(roots_ref.at[seq], owned_ref.at[seq], own_sem.at[3]),
    )
    for copy in own_copies:
        copy.start()
    for d in range(1, 8):
        far(0, d, tokens_ref, x_in).start()
    for k, to in enumerate(small_ids):
        small_copy(k, to).start()

    def head_loads(u):
        at = u * HEAD if isinstance(u, int) else pl.multiple_of(u * HEAD, HEAD)
        return [
            pltpu.make_async_copy(
                weights_ref.at[:, pl.ds(at, HEAD)],
                heads.at[u, pl.ds(mine, 256)],
                load_sem.at[u],
            )
        ]

    def trio_loads(k, sem):
        first = n_heads * HEAD
        return [
            pltpu.make_async_copy(
                weights_ref.at[
                    :,
                    pl.ds(
                        pl.multiple_of(first + part * n_trios * TRIO + k * TRIO, TRIO), TRIO
                    ),
                ],
                trios.at[k, pl.ds(mine, 256), pl.ds(part * TRIO, TRIO)],
                load_sem.at[n_heads + part * n_trios + k],
            )
            for part in range(3)
        ]

    def remote(flow, buf, i, unit, first, rows, to):
        piece = buf.at[i, pl.ds(pl.multiple_of(first, 16), rows)]
        return pltpu.make_async_remote_copy(
            src_ref=piece,
            dst_ref=piece,
            send_sem=send_sem.at[flow, unit],
            recv_sem=recv_sem.at[flow, unit],
            device_id=to,
            device_id_type=MESH,
        )

    def copies(buf, i, unit):
        near = mine + quarter * 64
        wide = mine + (3 - quarter) * 64
        got = theirs + quarter * 64
        other = mine + (quarter + 1 - 2 * (z % 2)) * 64 + 48
        table = {
            "core": (0, mine, 256, core_id),
            "near": (1, near, 64, y_id),
            "wide": (2, wide, 64, y_id),
            "x": (3, got, 64, x_id),
            "z": (4, got, 48, z_id),
            "rest": (6, other, 16, y_id),
            "pass": (5, theirs, 256, core_id),
        }

        def pick(name):
            flow, first, rows, to = table[name]
            return remote(flow, buf, i, unit, first, rows, to)

        return pick

    def head(u):
        return copies(heads, u, u)

    def trio(k):
        return copies(trios, k, n_heads + k)

    def send_first(c3):
        c3("near").start()
        c3("wide").start()
        c3("rest").start()
        c3("core").start()

    def send_on(c3):
        c3("near").wait()
        c3("x").start()
        c3("z").start()

    def hand_over(c3):
        c3("wide").wait()
        c3("rest").wait()
        c3("x").wait()
        c3("z").wait()
        c3("pass").start()

    def arrived(c3):
        c3("core").wait()
        c3("pass").wait()

    for u in range(n_heads):
        for copy in head_loads(u):
            copy.start()

    def load_trio(k, carry):
        for copy in trio_loads(k, None):
            copy.start()
        return carry

    lax.fori_loop(0, n_trios, load_trio, 0)
    for u in range(n_heads):
        for copy in head_loads(u):
            copy.wait()
        send_first(head(u))

    def first_trio(k, carry):
        for copy in trio_loads(k, None):
            copy.wait()
        send_first(trio(k))
        return carry

    lax.fori_loop(0, n_trios, first_trio, 0)
    send_on(head(0))
    send_on(head(1))

    def turn(source, r, wait):
        copy = pltpu.make_async_copy(turned, lefts_ref.at[r], out_sem.at[0])
        if wait:
            copy.wait()
        for j in range(8):
            turned[j * 128 : (j + 1) * 128, :] = source[:, j * 128 : (j + 1) * 128].T
        copy.start()

    for d in range(1, 8):
        far(0, d, tokens_ref, x_in).wait()
    own_copies[0].wait()
    for k, to in enumerate(small_ids):
        small_copy(k, to).wait()
    own_copies[2].wait()
    gain_one = smalls[0:1, :].astype(jnp.float32)
    for k in range(8):
        rows = slice(k * 64, (k + 1) * 64)
        unit = x_in[deal_ref[k]]
        xs[rows] = unit
        value = unit.astype(jnp.float32)
        xn[rows] = (value * rms_scale(value) * gain_one).astype(bf16)
    turn(xn, 0, False)

    def mixer_unit(u):
        proj[:, u * HEAD : (u + 1) * HEAD] = jnp.dot(
            xn[...], heads[u], preferred_element_type=jnp.float32
        )

    for u in range(n_heads + 2):
        if 2 <= u < n_heads:
            send_on(head(u))
        if u < 7:
            far(1, u + 1, dy_ref, dy_in).start()
        if u >= 1 and u - 1 < n_heads:
            hand_over(head(u - 1))
        if u >= 2:
            arrived(head(u - 2))
            if u - 2 < 6:
                mixer_unit(u - 2)

    out_proj = pltpu.make_async_copy(proj, proj_ref, out_sem.at[1])
    out_proj.start()
    width = D
    halo = slice(0, 8)
    for i in range(4):
        rows = slice(i * 128, (i + 1) * 128)
        back[8 + i * 128 : 8 + (i + 1) * 128] = proj[rows, :width] * proj[rows, 2 * width :]
    ring = pltpu.make_async_remote_copy(
        src_ref=back.at[pl.ds(512, 8)],
        dst_ref=mixed,
        send_sem=halo_sem.at[0],
        recv_sem=halo_sem.at[1],
        device_id=far_ids[0],
        device_id_type=MESH,
    )
    ring.start()
    send_on(trio(0))
    for d in range(1, 8):
        far(1, d, dy_ref, dy_in).wait()
    own_copies[1].wait()
    for k in range(8):
        dys[k * 64 : (k + 1) * 64] = dy_in[deal_ref[k]]
    turn(dys, 3, True)
    ring.wait()
    back[halo] = mixed[...]
    taps = [smalls[2 + k : 3 + k, :].astype(jnp.float32) for k in range(3)]
    for i in range(8):
        first = i * 64
        rows = slice(first, first + 64)
        conv = (
            taps[0] * masks_ref[0, rows] * back[first + 6 : first + 70]
            + taps[1] * masks_ref[1, rows] * back[first + 7 : first + 71]
            + taps[2] * back[first + 8 : first + 72]
        )
        yc[rows] = (proj[rows, width : 2 * width] * conv).astype(bf16)
    hand_over(trio(0))
    for u in range(6, n_heads):
        lanes = slice((u - 6) * HEAD, (u - 5) * HEAD)
        total[:, lanes] = xs[:, lanes].astype(jnp.float32) + jnp.dot(
            yc[...], heads[u], preferred_element_type=jnp.float32
        )
    out_h = pltpu.make_async_copy(total, h_ref, out_sem.at[2])
    out_h.start()
    gain_two = smalls[1:2, :].astype(jnp.float32)
    for i in range(8):
        rows = slice(i * 64, (i + 1) * 64)
        value = total[rows]
        hn[rows] = (value * rms_scale(value) * gain_two).astype(bf16)
    for i in range(4):
        back[i * 128 : (i + 1) * 128] = jnp.zeros((128, width), jnp.float32)
    send_on(trio(1))
    turn(yc, 1, True)
    out_h.wait()

    def act_copies(k, slot):
        at = pl.multiple_of(k * TRIO, TRIO)
        up = pl.multiple_of((n_trios + k) * TRIO, TRIO)
        return (
            pltpu.make_async_copy(
                act_buf.at[slot], act_ref.at[:, pl.ds(at, TRIO)], act_sem.at[slot, 0]
            ),
            pltpu.make_async_copy(
                d_gu_buf.at[slot, :, pl.ds(0, TRIO)],
                d_gu_ref.at[:, pl.ds(at, TRIO)],
                act_sem.at[slot, 1],
            ),
            pltpu.make_async_copy(
                d_gu_buf.at[slot, :, pl.ds(TRIO, TRIO)],
                d_gu_ref.at[:, pl.ds(up, TRIO)],
                act_sem.at[slot, 2],
            ),
        )

    def ffn(k, carry):
        pl.when(k + 2 < n_trios)(lambda: send_on(trio(k + 2)))
        pl.when(k + 1 < n_trios)(lambda: hand_over(trio(k + 1)))
        arrived(trio(k))
        pl.when(k < 7)(lambda: far(2, k + 1, roots_ref, owned_ref).start())
        slot = lax.rem(k, 2)

        @pl.when(k >= 2)
        def _():
            for copy in act_copies(k - 2, slot):
                copy.wait()

        gate = jnp.dot(hn[...], trios[k, :, :TRIO], preferred_element_type=jnp.float32)
        upper = jnp.dot(
            hn[...], trios[k, :, TRIO : 2 * TRIO], preferred_element_type=jnp.float32
        )
        d_act = jnp.dot(dys[...], trios[k, :, 2 * TRIO :], preferred_element_type=jnp.float32)
        sig = jax.nn.sigmoid(gate)
        silu = gate * sig
        act_buf[slot] = (silu * upper).astype(bf16)
        d_gu_buf[slot, :, :TRIO] = (
            d_act * upper * sig * (1.0 + gate * (1.0 - sig))
        ).astype(bf16)
        d_gu_buf[slot, :, TRIO:] = (d_act * silu).astype(bf16)
        for copy in act_copies(k, slot):
            copy.start()
        total[...] += contract_cols(act_buf[slot], trios[k, :, 2 * TRIO :])
        back[0:512] += contract_cols(d_gu_buf[slot], trios[k, :, : 2 * TRIO])
        return carry

    lax.fori_loop(0, n_trios, ffn, 0)
    turn(hn, 2, True)
    out_back = pltpu.make_async_copy(back.at[pl.ds(0, 512)], d_hn_ref, out_sem.at[3])
    out_back.start()
    yc[...] = total[...].astype(bf16)
    last = (
        pltpu.make_async_copy(yc, result_ref, out_sem.at[4]),
        pltpu.make_async_copy(xs, x_ref, out_sem.at[5]),
        pltpu.make_async_copy(dys, dy_out_ref, out_sem.at[6]),
        pltpu.make_async_copy(smalls, smalls_ref, out_sem.at[7]),
        pltpu.make_async_copy(mixed, prev_ref, out_sem.at[8]),
        pltpu.make_async_copy(heads, heads_ref, out_sem.at[9]),
    )
    for copy in last:
        copy.start()
    for k in range(n_trios - 2, n_trios):
        for copy in act_copies(k, k % 2):
            copy.wait()
    for copy in last:
        copy.wait()
    for d in range(1, 8):
        far(2, d, roots_ref, owned_ref).wait()
    own_copies[3].wait()
    out_proj.wait()
    out_back.wait()
    pltpu.make_async_copy(turned, lefts_ref.at[2], out_sem.at[0]).wait()


def gathered_forward(deal_order, tokens, dys, weights, small, masks, roots):
    bf16, f32 = jnp.bfloat16, jnp.float32
    rows = tokens.shape[0] * tokens.shape[1]
    n_heads = 4 * D // HEAD
    n_trios = FF // TRIO
    count = n_heads + n_trios
    anywhere = pl.BlockSpec(memory_space=pl.ANY)
    vmem = pl.BlockSpec(memory_space=pltpu.VMEM)
    shape = jax.ShapeDtypeStruct
    return pl.pallas_call(
        forward_kernel,
        out_shape=(
            shape((4, D, rows), bf16),
            shape((rows, D), bf16),
            shape((rows, D), bf16),
            shape((rows, 3 * D), f32),
            shape((8, D), f32),
            shape((rows, D), f32),
            shape((rows, FF), bf16),
            shape((rows, 2 * FF), bf16),
            shape((rows, D), f32),
            shape((rows, D), bf16),
            shape((n_heads, D, HEAD), bf16),
            shape((8, D), bf16),
            shape(roots.shape, bf16),
        ),
        in_specs=[
            pl.BlockSpec(memory_space=pltpu.SMEM),
            anywhere,
            anywhere,
            anywhere,
            vmem,
            vmem,
            anywhere,
        ],
        out_specs=(anywhere,) * 13,
        scratch_shapes=[
            pltpu.VMEM(tokens.shape, bf16),
            pltpu.VMEM(tokens.shape, bf16),
            pltpu.VMEM((n_heads, D, HEAD), bf16),
            pltpu.VMEM((n_trios, D, 3 * TRIO), bf16),
            pltpu.VMEM((8, D), bf16),
            pltpu.VMEM((rows, D), bf16),
            pltpu.VMEM((rows, D), bf16),
            pltpu.VMEM((rows, D), bf16),
            pltpu.VMEM((rows, D), bf16),
            pltpu.VMEM((rows, D), bf16),
            pltpu.VMEM((D, rows), bf16),
            pltpu.VMEM((rows, 3 * D), f32),
            pltpu.VMEM((8, D), f32),
            pltpu.VMEM((rows, D), f32),
            pltpu.VMEM((rows + 8, D), f32),
            pltpu.VMEM((2, rows, TRIO), bf16),
            pltpu.VMEM((2, rows, 2 * TRIO), bf16),
            pltpu.SemaphoreType.DMA((4,)),
            pltpu.SemaphoreType.DMA((n_heads + 3 * n_trios,)),
            pltpu.SemaphoreType.DMA((3, 7)),
            pltpu.SemaphoreType.DMA((3, 7)),
            pltpu.SemaphoreType.DMA((3,)),
            pltpu.SemaphoreType.DMA((3,)),
            pltpu.SemaphoreType.DMA((7, count)),
            pltpu.SemaphoreType.DMA((7, count)),
            pltpu.SemaphoreType.DMA((2,)),
            pltpu.SemaphoreType.DMA((10,)),
            pltpu.SemaphoreType.DMA((2, 3)),
        ],
        compiler_params=pltpu.CompilerParams(
            collective_id=1, has_side_effects=True, vmem_limit_bytes=63 << 20
        ),
        cost_estimate=pl.CostEstimate(
            flops=8 * rows * D * FF, bytes_accessed=10**8, transcendentals=0
        ),
        name="gathered_forward",
    )(deal_order, tokens, dys, weights, small, masks, roots)


PARTS = 7


def closing_kernel(
    grad_in, vec_in, terms_in, stats_in, update_in, state_in, grad, vec, state, step, stats, update
):
    grad[...] = grad_in[...].astype(jnp.float32)
    stats[...] = BETA * stats_in[...] + ((1.0 - BETA) / BLK) * terms_in[...].astype(jnp.float32)
    for i in range(update_in.shape[0]):
        for m in range(update_in.shape[1]):
            update[i, :, m] = -LEARN * update_in[i, m].astype(jnp.float32)

    @pl.when(pl.program_id(0) == 0)
    def _():
        count = vec.shape[0]
        turned = vec_in[:, :BLK].astype(jnp.float32).T[:count]
        fresh = BETA_VEC * state_in[...] + (1.0 - BETA_VEC) * turned * turned
        vec[...] = turned
        state[...] = fresh
        step[...] = -LEARN_VEC * turned * lax.rsqrt(fresh)


def closing(grad_bf, terms, kron_stats, update, vector_state):
    f32 = jnp.float32
    rows, wide = grad_bf.shape
    columns = wide - COLS
    kinds, blocks, share, _ = kron_stats.shape
    nrow, ncol = rows // BLK, columns // BLK
    shape = jax.ShapeDtypeStruct
    vec_spec = pl.BlockSpec(vector_state.shape, lambda g: (0, 0))
    grad_spec = pl.BlockSpec((rows, columns // PARTS), lambda g: (0, g))
    stat_spec = pl.BlockSpec((kinds, blocks // PARTS, share, BLK), lambda g: (0, g, 0, 0))
    groups = ncol // 4
    outs = pl.pallas_call(
        closing_kernel,
        grid=(PARTS,),
        out_shape=(
            shape((rows, columns), f32),
            shape(vector_state.shape, f32),
            shape(vector_state.shape, f32),
            shape(vector_state.shape, f32),
            shape(kron_stats.shape, f32),
            shape((nrow, groups, 4, share, BLK), f32),
        ),
        in_specs=[
            grad_spec,
            pl.BlockSpec((rows, COLS), lambda g: (0, columns // COLS)),
            stat_spec,
            stat_spec,
            pl.BlockSpec((nrow, 4, groups // PARTS, share, BLK), lambda g: (0, 0, g, 0, 0)),
            vec_spec,
        ],
        out_specs=(
            grad_spec,
            vec_spec,
            vec_spec,
            vec_spec,
            stat_spec,
            pl.BlockSpec((nrow, groups // PARTS, 4, share, BLK), lambda g: (0, g, 0, 0, 0)),
        ),
        compiler_params=pltpu.CompilerParams(vmem_limit_bytes=40 << 20),
        name="closing",
    )(
        grad_bf,
        grad_bf,
        terms.reshape(kron_stats.shape),
        kron_stats,
        update.reshape(nrow, 4, groups, share, BLK),
        vector_state,
    )
    return (*outs[:5], outs[5].reshape(blocks, share, BLK))


def contract_units(left, units):
    return sum(
        contract_cols(left[:, u * HEAD : (u + 1) * HEAD], units[u]) for u in range(units.shape[0])
    )


def shards(
    tokens_in,
    out_grad,
    deal_order,
    seq_lengths,
    weights,
    norm_gains,
    conv_kernel,
    vector_state,
    kron_stats,
    kron_roots,
):
    n_seq = lax.axis_size("seq")
    n_wsh = lax.axis_size("wsh")
    rows = tokens_in.shape[1]
    unit = rows // n_seq
    first_row = lax.axis_index("seq") * rows
    pos = seq_positions(seq_lengths[0], first_row, rows + 2)
    masks = [(pos >= 2 - k).astype(jnp.float32)[:, None] for k in range(3)]
    nrow_blocks, ncol_blocks = weights.shape[0] // BLK, weights.shape[1] // BLK
    share = BLK // n_seq
    roots = kron_roots.astype(jnp.bfloat16).reshape(
        2, nrow_blocks, ncol_blocks // 4, 4, share, BLK
    )
    roots = roots.transpose(1, 3, 0, 2, 4, 5).reshape(n_seq, 2, ncol_blocks // 4, share, BLK)
    small = jnp.concatenate(
        [norm_gains, conv_kernel, jnp.zeros((3, norm_gains.shape[1]), jnp.bfloat16)], axis=0
    )
    (
        lefts,
        x_bf,
        dy_bf,
        proj,
        prev,
        hidden_sum,
        act,
        d_gu,
        d_hn,
        result,
        heads,
        smalls,
        owned,
    ) = gathered_forward(
        deal_order,
        tokens_in.reshape(n_seq, unit, D),
        out_grad.reshape(n_seq, unit, D),
        weights,
        small,
        jnp.stack([masks[0][:rows], masks[1][:rows]]),
        roots,
    )
    gains = smalls[:2].astype(jnp.float32)
    kernel = smalls[2:5].astype(jnp.float32)
    xf = x_bf.astype(jnp.float32)
    scale_one = rms_scale(xf)
    scale_two = rms_scale(hidden_sum)
    b_part = proj[:, :D]
    c_part = proj[:, D : 2 * D]
    x_part = proj[:, 2 * D :]
    ext = jnp.concatenate([prev[6:], b_part * x_part], axis=0)
    conv = (
        kernel[0] * masks[0][:rows] * ext[0:rows]
        + kernel[1] * masks[1][:rows] * ext[1 : rows + 1]
        + kernel[2] * masks[2][:rows] * ext[2 : rows + 2]
    )
    d_norm_two, g_gain_two = norm_back(d_hn, hidden_sum, scale_two, gains[1])
    d_hidden = dy_bf.astype(jnp.float32) + d_norm_two
    d_mix = d_hidden.astype(jnp.bfloat16)
    d_yc = contract_units(d_mix, heads[3 * D // HEAD :])
    d_c = d_yc * conv
    d_conv = d_yc * c_part
    after = passed_along(d_conv[:2], "seq", -1)
    d_ext = jnp.concatenate([d_conv, after], axis=0)
    weighted = [d_ext * masks[k] for k in range(3)]
    d_bx = (
        kernel[2] * weighted[2][:rows]
        + kernel[1] * weighted[1][1 : rows + 1]
        + kernel[0] * weighted[0][2 : rows + 2]
    )
    g_taps = jnp.stack([jnp.sum(weighted[k][:rows] * ext[k : k + rows], axis=0) for k in range(3)])
    d_proj = jnp.concatenate([d_bx * x_part, d_c, d_bx * b_part], axis=1).astype(jnp.bfloat16)
    d_xn = contract_units(d_proj, heads[: 3 * D // HEAD])
    d_norm_one, g_gain_one = norm_back(d_xn, xf, scale_one, gains[0])
    d_input = (d_hidden + d_norm_one).astype(jnp.bfloat16)
    g_vec = jnp.concatenate([g_gain_one[None], g_gain_two[None], g_taps], axis=0)
    inverse = jnp.argsort(deal_order)
    result_leaving = jnp.take(result.reshape(n_seq, unit, D), inverse, axis=0)
    leaving = jnp.take(d_input.reshape(n_seq, unit, D), inverse, axis=0)
    vec = jnp.pad(g_vec.T.astype(jnp.bfloat16), ((0, 0), (0, COLS - g_vec.shape[0])))
    grad_bf, terms, update, out_back, dx_back = reduced(
        lefts,
        (d_proj, d_mix, d_gu, act),
        vec.reshape(n_wsh, D // n_wsh, COLS),
        owned,
        (result_leaving, leaving),
        float((rows * n_seq * n_wsh) ** -0.5),
    )
    grad_shard, vec_grad, state_new, vec_update, stats_new, update = closing(
        grad_bf, terms, kron_stats, update, vector_state
    )
    return (
        out_back.reshape(1, rows, D),
        dx_back.reshape(1, rows, D),
        grad_shard,
        vec_grad,
        state_new,
        vec_update,
        stats_new,
        update,
    )


def solution(mesh):
    known = mesh.shape["seq"] == 8 and mesh.shape["wsh"] == 4
    return jax.shard_map(
        shards if known else plain_shards,
        mesh=mesh,
        in_specs=(
            P("wsh", "seq", None),
            P("wsh", "seq", None),
            P(),
            P("wsh", None),
            P("wsh", None),
            P(None, "wsh"),
            P(None, "wsh"),
            P(None, "wsh"),
            P(None, "wsh", "seq", None),
            P(None, "wsh", "seq", None),
        ),
        out_specs=(
            P("wsh", "seq", None),
            P("wsh", "seq", None),
            P("wsh", None),
            P(None, "wsh"),
            P(None, "wsh"),
            P(None, "wsh"),
            P(None, "wsh", "seq", None),
            P("wsh", "seq", None),
        ),
        check_vma=False,
    )
```

```python
import functools

import jax
import jax.numpy as jnp
from jax import lax
from jax.experimental import pallas as pl
from jax.experimental.pallas import tpu as pltpu
from jax.sharding import PartitionSpec as P

MESH = pl.DeviceIdType.MESH

D = 1024
FF = 4608
BLK = 128


EPS = 1e-05
BETA = 0.5
BETA_VEC = 0.5
LEARN = 0.03
LEARN_VEC = 0.05
HIGH = lax.Precision.HIGHEST


def passed_along(block, axis, distance):
    devices = range(lax.axis_size(axis))
    route = [(i - distance, i) for i in devices if i - distance in devices]
    return lax.ppermute(block, axis, route)


def seq_positions(lengths_row, first, count):
    starts = jnp.cumsum(lengths_row) - lengths_row
    rows_at = first + jnp.arange(count, dtype=jnp.int32)
    begin = jnp.max(jnp.where(starts[None, :] <= rows_at[:, None], starts[None, :], 0), axis=1)
    return rows_at - begin


def rms_scale(values):
    return lax.rsqrt(jnp.mean(values * values, axis=1, keepdims=True) + EPS)


def norm_back(upstream, values, scale, gain):
    scaled = upstream * gain
    inner = jnp.mean(scaled * values, axis=1, keepdims=True)
    return (
        scale * scaled - values * scale * scale * scale * inner,
        jnp.sum(upstream * values * scale, axis=0),
    )


def contract_rows(left, right):
    return lax.dot_general(
        left, right, (((0,), (0,)), ((), ())), preferred_element_type=jnp.float32
    )


def contract_cols(left, right):
    return lax.dot_general(
        left, right, (((1,), (1,)), ((), ())), preferred_element_type=jnp.float32
    )


def plain_shards(
    tokens_in,
    out_grad,
    deal_order,
    seq_lengths,
    weights,
    norm_gains,
    conv_kernel,
    vector_state,
    kron_stats,
    kron_roots,
):
    n_seq = lax.axis_size("seq")
    n_wsh = lax.axis_size("wsh")
    rows = tokens_in.shape[1]
    unit = rows // n_seq
    arrived = (
        lax.all_to_all(
            tokens_in.reshape(n_seq, unit, D), "seq", split_axis=0, concat_axis=0, tiled=True
        ),
        lax.all_to_all(
            out_grad.reshape(n_seq, unit, D), "seq", split_axis=0, concat_axis=0, tiled=True
        ),
    )
    x_bf = jnp.take(arrived[0], deal_order, axis=0).reshape(rows, D)
    dy_bf = jnp.take(arrived[1], deal_order, axis=0).reshape(rows, D)
    full_w, gains_bf, kernel_bf = (
        lax.all_gather(weights, "wsh", axis=0, tiled=True),
        lax.all_gather(norm_gains, "wsh", axis=1, tiled=True),
        lax.all_gather(conv_kernel, "wsh", axis=1, tiled=True),
    )
    gains = gains_bf.astype(jnp.float32)
    kernel = kernel_bf.astype(jnp.float32)
    first_row = lax.axis_index("seq") * rows
    pos = seq_positions(seq_lengths[0], first_row, rows + 2)
    masks = [(pos >= 2 - k).astype(jnp.float32)[:, None] for k in range(3)]
    xf = x_bf.astype(jnp.float32)
    scale_one = rms_scale(xf)
    xn = (xf * scale_one * gains[0]).astype(jnp.bfloat16)
    proj = jnp.dot(xn, full_w[:, : 3 * D], preferred_element_type=jnp.float32)
    b_part = proj[:, :D]
    c_part = proj[:, D : 2 * D]
    x_part = proj[:, 2 * D :]
    conv_in = b_part * x_part
    prev = passed_along(conv_in[rows - 2 :], "seq", 1)
    ext = jnp.concatenate([prev, conv_in], axis=0)
    conv = (
        kernel[0] * masks[0][:rows] * ext[0:rows]
        + kernel[1] * masks[1][:rows] * ext[1 : rows + 1]
        + kernel[2] * masks[2][:rows] * ext[2 : rows + 2]
    )
    yc = (c_part * conv).astype(jnp.bfloat16)
    hidden_sum = xf + jnp.dot(yc, full_w[:, 3 * D : 4 * D], preferred_element_type=jnp.float32)
    scale_two = rms_scale(hidden_sum)
    hn = (hidden_sum * scale_two * gains[1]).astype(jnp.bfloat16)
    gate_up = jnp.dot(hn, full_w[:, 4 * D : 4 * D + 2 * FF], preferred_element_type=jnp.float32)
    gate = gate_up[:, :FF]
    upper = gate_up[:, FF:]
    sig = jax.nn.sigmoid(gate)
    act = (gate * sig * upper).astype(jnp.bfloat16)
    ffn = contract_cols(act, full_w[:, 4 * D + 2 * FF :])
    result = (hidden_sum + ffn).astype(jnp.bfloat16)
    g_down = contract_rows(dy_bf, act)
    d_act = jnp.dot(dy_bf, full_w[:, 4 * D + 2 * FF :], preferred_element_type=jnp.float32)
    d_gate = d_act * upper * sig * (1.0 + gate * (1.0 - sig))
    d_upper = d_act * gate * sig
    d_gu = jnp.concatenate([d_gate, d_upper], axis=1).astype(jnp.bfloat16)
    g_gu = contract_rows(hn, d_gu)
    d_hn = contract_cols(d_gu, full_w[:, 4 * D : 4 * D + 2 * FF])
    d_norm_two, g_gain_two = norm_back(d_hn, hidden_sum, scale_two, gains[1])
    d_hidden = dy_bf.astype(jnp.float32) + d_norm_two
    d_mix = d_hidden.astype(jnp.bfloat16)
    g_out = contract_rows(yc, d_mix)
    d_yc = contract_cols(d_mix, full_w[:, 3 * D : 4 * D])
    d_c = d_yc * conv
    d_conv = d_yc * c_part
    after = passed_along(d_conv[:2], "seq", -1)
    d_ext = jnp.concatenate([d_conv, after], axis=0)
    weighted = [d_ext * masks[k] for k in range(3)]
    d_bx = (
        kernel[2] * weighted[2][:rows]
        + kernel[1] * weighted[1][1 : rows + 1]
        + kernel[0] * weighted[0][2 : rows + 2]
    )
    g_taps = jnp.stack([jnp.sum(weighted[k][:rows] * ext[k : k + rows], axis=0) for k in range(3)])
    d_proj = jnp.concatenate([d_bx * x_part, d_c, d_bx * b_part], axis=1).astype(jnp.bfloat16)
    g_in = contract_rows(xn, d_proj)
    d_xn = contract_cols(d_proj, full_w[:, : 3 * D])
    d_norm_one, g_gain_one = norm_back(d_xn, xf, scale_one, gains[0])
    d_input = (d_hidden + d_norm_one).astype(jnp.bfloat16)
    g_vec = jnp.concatenate([g_gain_one[None], g_gain_two[None], g_taps], axis=0)
    inverse = jnp.argsort(deal_order)
    leaving = (
        jnp.take(result.reshape(n_seq, unit, D), inverse, axis=0),
        jnp.take(d_input.reshape(n_seq, unit, D), inverse, axis=0),
    )
    returned = (
        lax.all_to_all(leaving[0], "seq", split_axis=0, concat_axis=0, tiled=True),
        lax.all_to_all(leaving[1], "seq", split_axis=0, concat_axis=0, tiled=True),
    )
    summed = (
        lax.psum_scatter(g_in.astype(jnp.bfloat16), "wsh", scatter_dimension=0, tiled=True).astype(
            jnp.float32
        ),
        lax.psum_scatter(g_out.astype(jnp.bfloat16), "wsh", scatter_dimension=0, tiled=True).astype(
            jnp.float32
        ),
        lax.psum_scatter(g_gu.astype(jnp.bfloat16), "wsh", scatter_dimension=0, tiled=True).astype(
            jnp.float32
        ),
        lax.psum_scatter(
            g_down.astype(jnp.bfloat16), "wsh", scatter_dimension=0, tiled=True
        ).astype(jnp.float32),
        lax.psum_scatter(g_vec.astype(jnp.bfloat16), "wsh", scatter_dimension=1, tiled=True).astype(
            jnp.float32
        ),
    )
    summed = (
        lax.psum(summed[0].astype(jnp.bfloat16), "seq").astype(jnp.float32),
        lax.psum(summed[1].astype(jnp.bfloat16), "seq").astype(jnp.float32),
        lax.psum(summed[2].astype(jnp.bfloat16), "seq").astype(jnp.float32),
        lax.psum(summed[3].astype(jnp.bfloat16), "seq").astype(jnp.float32),
        lax.psum(summed[4].astype(jnp.bfloat16), "seq").astype(jnp.float32),
    )
    grad_scale = lax.rsqrt(jnp.asarray(rows * n_seq * n_wsh, jnp.float32))
    grad_shard = jnp.concatenate([summed[0], summed[1], summed[2], summed[3]], axis=1) * grad_scale
    vec_grad = summed[4] * grad_scale
    state_new = BETA_VEC * vector_state + (1.0 - BETA_VEC) * vec_grad * vec_grad
    vec_update = -LEARN_VEC * vec_grad * lax.rsqrt(state_new)
    nrow_blocks = grad_shard.shape[0] // BLK
    ncol_blocks = grad_shard.shape[1] // BLK
    grad_blocks = (
        grad_shard.reshape(nrow_blocks, BLK, ncol_blocks, BLK)
        .transpose(0, 2, 1, 3)
        .reshape(nrow_blocks * ncol_blocks, BLK, BLK)
    )
    share = BLK // n_seq
    first_block_row = lax.axis_index("seq") * share
    block_rows = lax.dynamic_slice_in_dim(grad_blocks, first_block_row, share, 1)
    block_cols = lax.dynamic_slice_in_dim(grad_blocks, first_block_row, share, 2)
    left_term = jnp.einsum("nij,nkj->nik", block_rows, grad_blocks, precision=HIGH)
    right_term = jnp.einsum("nji,njk->nik", block_cols, grad_blocks, precision=HIGH)
    stats_new = jnp.stack(
        [
            BETA * kron_stats[0] + (1.0 - BETA) * left_term / BLK,
            BETA * kron_stats[1] + (1.0 - BETA) * right_term / BLK,
        ]
    )
    right_full = lax.all_gather(
        kron_roots[1].astype(jnp.bfloat16), "seq", axis=1, tiled=True
    ).astype(jnp.float32)
    left_mul = jnp.einsum("nij,njk->nik", kron_roots[0], grad_blocks, precision=HIGH)
    update = -LEARN * jnp.einsum("nij,njk->nik", left_mul, right_full, precision=HIGH)
    return (
        returned[0].reshape(1, rows, D),
        returned[1].reshape(1, rows, D),
        grad_shard,
        vec_grad,
        state_new,
        vec_update,
        stats_new,
        update,
    )


COLS = 256
GAP = 2
RING = 14
SEMS = 4
BATCHES = 5


def place():
    seq, wsh = lax.axis_index("seq"), lax.axis_index("wsh")
    return seq // 2, seq % 2, wsh // 2, wsh % 2


def reduce_kernel(
    edges,
    scale,
    inverse_ref,
    lefts_ref,
    d_gu_ref,
    act_ref,
    smalls_ref,
    masks_ref,
    x_ref,
    dy_ref,
    proj_ref,
    prev_ref,
    h_ref,
    d_hn_ref,
    heads_ref,
    owned_ref,
    leave_ref,
    grad_ref,
    terms_ref,
    update_ref,
    arrive_ref,
    arrive_two_ref,
    b_buf,
    g_buf,
    core_in,
    y_out,
    y_in,
    x_out,
    x_in,
    pair_out,
    pair_in,
    far_out,
    far_in,
    final,
    r_buf,
    t_buf,
    u_buf,
    b_sem,
    r_sem,
    o_sem,
    t_sem,
    send_sem,
    recv_sem,
    far_send,
    far_recv,
    own_sem,
    back_send,
    back_recv,
    x_buf,
    dy_buf,
    proj,
    product_in,
    h_buf,
    d_hidden,
    heads,
    d_conv,
    d_proj,
    d_mix,
    leave_buf,
    vec_buf,
    fetch_sem,
    halo_sem,
):
    z, x, y, c = place()
    seq, wsh = lax.axis_index("seq"), lax.axis_index("wsh")
    n_real = edges[-1]
    count = n_real + 1
    core_id = (seq, y * 2 + (1 - c))
    y_id = (seq, (1 - y) * 2 + c)
    x_id = (z * 2 + (1 - x), wsh)
    high, low = z // 2, z % 2
    pair_id = ((2 * high + 1 - low) * 2 + x, wsh)
    over_id = ((2 * (1 - high) + low) * 2 + x, wsh)
    owned_row = x * 128 + low * 64 + high * 32
    far_ids = [(lax.rem(seq + d, 8), wsh) for d in range(1, 8)]

    barrier = pltpu.get_barrier_semaphore()
    for device in [core_id, y_id] + far_ids:
        pl.semaphore_signal(barrier, inc=1, device_id=device, device_id_type=MESH)
    pl.semaphore_wait(barrier, 9)

    def far(k, d):
        source, target = own_pairs[k]
        to = far_ids[d - 1]
        return pltpu.make_async_remote_copy(
            src_ref=source.at[to[0]],
            dst_ref=target.at[seq],
            send_sem=far_send.at[k, d - 1],
            recv_sem=far_recv.at[k, d - 1],
            device_id=to,
            device_id_type=MESH,
        )

    own_pairs = ((leave_ref, arrive_ref), (leave_buf, arrive_two_ref))

    def own_copy(k):
        source, target = own_pairs[k]
        return pltpu.make_async_copy(source.at[seq], target.at[seq], own_sem.at[k])

    own_copy(0).start()
    for d in range(1, 8):
        far(0, d).start()
    fetches = [
        pltpu.make_async_copy(source, target, fetch_sem.at[k])
        for k, (source, target) in enumerate(
            (
                (h_ref, h_buf),
                (d_hn_ref, d_hidden),
                (dy_ref, dy_buf),
                (proj_ref, proj),
                (prev_ref, product_in.at[pl.ds(0, 8)]),
                (heads_ref, heads),
                (x_ref, x_buf),
            )
        )
    ]
    for copy in fetches:
        copy.start()
    vec_buf[...] = jnp.zeros_like(vec_buf)

    batch = update_ref.shape[1] // BATCHES

    def u_piece(ref, device, b):
        return ref.at[device, pl.ds(b * batch, batch)]

    def u_back(b, d):
        to = far_ids[d - 1]
        return pltpu.make_async_remote_copy(
            src_ref=u_piece(u_buf, to[0], b),
            dst_ref=u_piece(update_ref, seq, b),
            send_sem=back_send.at[b, d - 1],
            recv_sem=back_recv.at[b, d - 1],
            device_id=to,
            device_id_type=MESH,
        )

    def u_own(b):
        return pltpu.make_async_copy(
            u_piece(u_buf, seq, b), u_piece(update_ref, seq, b), own_sem.at[2 + b]
        )

    def remote(flow, n, source, target, device):
        k = lax.rem(n, SEMS)
        return pltpu.make_async_remote_copy(
            src_ref=source,
            dst_ref=target,
            send_sem=send_sem.at[flow, k],
            recv_sem=recv_sem.at[flow, k],
            device_id=device,
            device_id_type=MESH,
        )

    def core_copy(n):
        slot = lax.rem(n, RING)
        return remote(0, n, g_buf.at[slot, 1 - c], core_in.at[slot], core_id)

    def y_copy(n):
        return remote(1, n, y_out.at[lax.rem(n, SEMS)], y_in.at[lax.rem(n, RING)], y_id)

    def x_copy(n):
        return remote(2, n, x_out.at[lax.rem(n, SEMS)], x_in.at[lax.rem(n, RING)], x_id)

    def pair_copy(n):
        return remote(
            3, n, pair_out.at[lax.rem(n, SEMS)], pair_in.at[lax.rem(n, RING)], pair_id
        )

    def over_copy(n):
        return remote(4, n, far_out.at[lax.rem(n, SEMS)], far_in.at[lax.rem(n, RING)], over_id)

    def final_rows(n, first, size):
        return final.at[lax.rem(n, RING), pl.ds(pl.multiple_of(first, size), size)]

    def over_share(n):
        piece = final_rows(n, owned_row, 32)
        return remote(5, n, piece, piece, over_id)

    def pair_share(n):
        piece = final_rows(n, x * 128 + low * 64, 64)
        return remote(6, n, piece, piece, pair_id)

    def x_share(n):
        piece = final_rows(n, x * 128, 128)
        return remote(7, n, piece, piece, x_id)

    def b_copies(n):
        slot = lax.rem(n, SEMS)
        column = n_real - 1 - n
        for r, source in enumerate((d_proj, d_mix, d_gu_ref, act_ref)):
            low, high = edges[r], edges[r + 1]
            at = jnp.clip(column - low, 0, high - low - 1)
            at = pl.multiple_of(at * COLS, COLS)
            copy = pltpu.make_async_copy(
                source.at[:, pl.ds(at, COLS)], b_buf.at[slot], b_sem.at[slot]
            )
            yield (column >= low) & (column < high), copy

    def r_copies(n):
        slot = lax.rem(n, SEMS)
        at = jnp.maximum(n_real - 1 - n, 0) // 2
        return [
            pltpu.make_async_copy(
                owned_ref.at[:, kind, at], r_buf.at[slot, kind], r_sem.at[slot, kind]
            )
            for kind in range(2)
        ]

    def has_block(n):
        return (n < n_real) & (lax.rem(n_real - 1 - n, 2) == lax.rem(seq, 4) // 2)

    def o_copy(n):
        at = pl.multiple_of(lax.rem(2 * n_real - n, n_real + 1) * COLS, COLS)
        return pltpu.make_async_copy(
            final.at[lax.rem(n, RING)], grad_ref.at[:, pl.ds(at, COLS)], o_sem.at[lax.rem(n, SEMS)]
        )

    def t_copy(n):
        slot = lax.rem(n, SEMS)
        at = pl.multiple_of(jnp.maximum(n_real - 1 - n, 0) * 2, 2)
        return pltpu.make_async_copy(
            t_buf.at[slot], terms_ref.at[:, :, pl.ds(at, 2)], t_sem.at[slot]
        )

    def wide(value):
        return value.astype(jnp.float32)

    def sum_rows(slot, first, size):
        rows = pl.ds(pl.multiple_of(first, size), size)
        total = wide(g_buf[slot, c, y, rows]) + wide(core_in[slot, y, rows])
        return total + wide(y_in[slot, rows])

    def sum_half(slot, row, size):
        rows = pl.ds(pl.multiple_of(row, size), size)
        return sum_rows(slot, x * 128 + row, size) + wide(x_in[slot, rows])

    def stage_load(n):
        for wanted, copy in b_copies(n):
            pl.when(wanted)(copy.start)

    def stage_product(n):
        slot = lax.rem(n, RING)
        column = n_real - 1 - n

        @pl.when(n < n_real)
        def _():
            for wanted, copy in b_copies(n):
                pl.when(wanted)(copy.wait)
            region = sum((column >= e).astype(jnp.int32) for e in edges[1:-1])
            right = b_buf[lax.rem(n, SEMS)]
            for w in range(4):
                product = jnp.dot(
                    lefts_ref[region, w * 256 : (w + 1) * 256, :],
                    right,
                    preferred_element_type=jnp.float32,
                )
                g_buf[slot, w % 2, w // 2] = product.astype(jnp.bfloat16)

        @pl.when(n == n_real)
        def _():
            for w in range(4):
                turned = vec_buf[:, w * 256 : (w + 1) * 256].T.astype(jnp.bfloat16)
                g_buf[slot, w % 2, w // 2, :, :BLK] = turned
                g_buf[slot, w % 2, w // 2, :, BLK:] = jnp.zeros_like(turned)

        core_copy(n).start()

    def stage_y(n):
        slot = lax.rem(n, RING)
        core_copy(n).wait()
        y_out[lax.rem(n, SEMS)] = (
            wide(g_buf[slot, c, 1 - y]) + wide(core_in[slot, 1 - y])
        ).astype(jnp.bfloat16)
        y_copy(n).start()

    def stage_x(n):
        slot = lax.rem(n, RING)
        y_copy(n).wait()
        x_out[lax.rem(n, SEMS)] = sum_rows(slot, (1 - x) * 128, 128).astype(jnp.bfloat16)
        x_copy(n).start()

    def stage_pair(n):
        slot = lax.rem(n, RING)
        x_copy(n).wait()
        total = sum_half(slot, (1 - low) * 64, 64)
        pair_out[lax.rem(n, SEMS)] = total.astype(jnp.bfloat16)
        pair_copy(n).start()

    def stage_over(n):
        slot = lax.rem(n, RING)
        pair_copy(n).wait()
        row = (1 - high) * 32
        total = sum_half(slot, low * 64 + row, 32)
        total = total + wide(pair_in[slot, pl.ds(pl.multiple_of(row, 32), 32)])
        far_out[lax.rem(n, SEMS)] = total.astype(jnp.bfloat16)
        over_copy(n).start()

    def stage_final(n):
        slot = lax.rem(n, RING)
        over_copy(n).wait()
        total = sum_half(slot, low * 64 + high * 32, 32)
        total = total + wide(pair_in[slot, pl.ds(pl.multiple_of(high * 32, 32), 32)])
        total = total + wide(far_in[slot])
        final[slot, pl.ds(pl.multiple_of(owned_row, 32), 32)] = (total * scale).astype(
            jnp.bfloat16
        )
        over_share(n).start()

    def stage_pair_share(n):
        over_share(n).wait()
        pair_share(n).start()

    def stage_share(n):
        pair_share(n).wait()
        x_share(n).start()

        @pl.when(has_block(n))
        def _():
            for copy in r_copies(n):
                copy.start()


    def stage_take(n):
        x_share(n).wait()
        o_copy(n).start()

    def stage_use(n):
        slot = lax.rem(n, RING)
        part = lax.rem(n, SEMS)

        @pl.when(n >= SEMS)
        def _():
            t_copy(n - SEMS).wait()

        @pl.when(n < n_real)
        def _():
            picked = lax.broadcasted_iota(jnp.int32, (16, BLK), 1) == (
                lax.broadcasted_iota(jnp.int32, (16, BLK), 0) + seq * 16
            )
            one_hot = picked.astype(jnp.float32).astype(jnp.bfloat16)
            for i in range(2):
                for j in range(2):
                    lanes = slice(j * BLK, (j + 1) * BLK)
                    block = final[slot, i * BLK : (i + 1) * BLK, lanes]
                    rows = final[
                        slot, pl.ds(pl.multiple_of(i * BLK + seq * 16, 16), 16), lanes
                    ]
                    first = contract_cols(jnp.concatenate([rows, one_hot], axis=0), block)
                    second = jnp.dot(
                        first[16:].astype(jnp.bfloat16),
                        block,
                        preferred_element_type=jnp.float32,
                    )
                    t_buf[part, 0, i, j] = first[:16].astype(jnp.bfloat16)
                    t_buf[part, 1, i, j] = second.astype(jnp.bfloat16)
            t_copy(n).start()

        @pl.when(has_block(n))
        def _():
            for copy in r_copies(n):
                copy.wait()
            block = final[
                slot,
                pl.ds(pl.multiple_of(seq // 4 * BLK, BLK), BLK),
                pl.ds(pl.multiple_of(lax.rem(seq, 2) * BLK, BLK), BLK),
            ]
            left = jnp.dot(
                r_buf[part, 0].reshape(BLK, BLK), block, preferred_element_type=jnp.float32
            )
            both = jnp.dot(
                left.astype(jnp.bfloat16),
                r_buf[part, 1].reshape(BLK, BLK),
                preferred_element_type=jnp.float32,
            )
            u_buf[:, (n_real - 1 - n) // 2] = both.astype(jnp.bfloat16).reshape(8, 16, BLK)

        column = n_real - 1 - n

        @pl.when((n < n_real) & (lax.rem(column, 2 * batch) == 0))
        def _():
            b = column // (2 * batch)
            u_own(b).start()
            for d in range(1, 8):
                u_back(b, d).start()

    def stage_done(n):
        o_copy(n).wait()

    offsets = {
        "load": 0,
        "product": GAP,
        "y": 2 * GAP,
        "x": 3 * GAP,
        "pair": 4 * GAP,
        "over": 5 * GAP,
        "final": 6 * GAP,
        "pair_share": 7 * GAP,
        "share": 8 * GAP,
        "take": 9 * GAP,
        "use": 9 * GAP,
        "done": 10 * GAP,
    }
    stages = (
        ("done", stage_done),
        ("take", stage_take),
        ("share", stage_share),
        ("pair_share", stage_pair_share),
        ("final", stage_final),
        ("over", stage_over),
        ("pair", stage_pair),
        ("x", stage_x),
        ("y", stage_y),
        ("product", stage_product),
        ("load", stage_load),
        ("use", stage_use),
    )

    width = D
    span = 128

    def gain(k):
        return smalls_ref[k : k + 1, :].astype(jnp.float32)

    def add_vec(k, value):
        vec_buf[k : k + 1, :] += jnp.sum(value, axis=0, keepdims=True)

    def shifted(ref, first, by):
        return ref[first + by : first + by + span]

    def back_norm_two(i):
        rows = slice(i * span, (i + 1) * span)
        if i == 0:
            for copy in fetches[:5]:
                copy.wait()
        value, up = h_buf[rows], d_hidden[rows]
        scale_two = rms_scale(value)
        scaled = up * gain(1)
        inner = jnp.mean(scaled * value, axis=1, keepdims=True)
        add_vec(1, up * value * scale_two)
        through = scale_two * scaled - value * scale_two * scale_two * scale_two * inner
        total = wide(dy_buf[rows]) + through
        d_hidden[rows] = total
        d_mix[rows] = total.astype(jnp.bfloat16)
        product_in[8 + i * span : 8 + (i + 1) * span] = (
            proj[rows, :width] * proj[rows, 2 * width :]
        )

    def back_out(i):
        lanes = slice(i * 256, (i + 1) * 256)
        if i == 0:
            fetches[5].wait()
        d_conv[0:512, lanes] = contract_cols(d_mix[:, :HEAD], heads[6, lanes]) + contract_cols(
            d_mix[:, HEAD:], heads[7, lanes]
        )

    ring = pltpu.make_async_remote_copy(
        src_ref=d_conv.at[pl.ds(0, 8)],
        dst_ref=d_conv.at[pl.ds(512, 8)],
        send_sem=halo_sem.at[0],
        recv_sem=halo_sem.at[1],
        device_id=far_ids[6],
        device_id_type=MESH,
    )

    def back_conv(i):
        rows = slice(i * span, (i + 1) * span)
        up = d_conv[rows]
        down = up * proj[rows, width : 2 * width]
        conv = jnp.zeros_like(up)
        for k in range(3):
            term = shifted(product_in, i * span, 6 + k)
            if k < 2:
                term = term * masks_ref[k, rows]
            conv = conv + gain(2 + k) * term
            add_vec(2 + k, down * term)
        d_proj[rows, width : 2 * width] = (up * conv).astype(jnp.bfloat16)
        d_conv[rows] = down
        if i == 0:
            ring.start()

    def back_taps(i):
        rows = slice(i * span, (i + 1) * span)
        if i == 3:
            ring.wait()
            tail = d_conv[512:520]
            d_conv[512:520] = jnp.where(seq == 7, jnp.zeros_like(tail), tail)
        first = i * span
        d_bx = (
            gain(4) * d_conv[rows]
            + gain(3) * shifted(masks_ref.at[1], first, 1) * shifted(d_conv, first, 1)
            + gain(2) * shifted(masks_ref.at[0], first, 2) * shifted(d_conv, first, 2)
        )
        d_proj[rows, :width] = (d_bx * proj[rows, 2 * width :]).astype(jnp.bfloat16)
        d_proj[rows, 2 * width :] = (d_bx * proj[rows, :width]).astype(jnp.bfloat16)

    def back_in(u):
        part = contract_cols(d_proj[:, u * HEAD : (u + 1) * HEAD], heads[u])
        if u == 0:
            h_buf[...] = part
        else:
            h_buf[...] += part

    def back_norm_one(i):
        rows = slice(i * span, (i + 1) * span)
        if i == 0:
            fetches[6].wait()
        value = jnp.concatenate([wide(x_buf[2 * i]), wide(x_buf[2 * i + 1])], axis=0)
        up = h_buf[rows]
        scale_one = rms_scale(value)
        scaled = up * gain(0)
        inner = jnp.mean(scaled * value, axis=1, keepdims=True)
        add_vec(0, up * value * scale_one)
        through = scale_one * scaled - value * scale_one * scale_one * scale_one * inner
        total = (d_hidden[rows] + through).astype(jnp.bfloat16)
        x_buf[2 * i] = total[:64]
        x_buf[2 * i + 1] = total[64:]

    def back_pick(i):
        for d in range(4 * i, 4 * i + 4):
            leave_buf[d] = x_buf[inverse_ref[d]]

    def back_leave(i):
        if i == 0:
            own_copy(1).start()
        far(1, i + 1).start()

    pieces = []
    for work, number, pause in (
        (back_norm_two, 4, 3),
        (back_out, 4, 0),
        (back_conv, 4, 0),
        (back_taps, 4, 4),
        (back_in, 6, 0),
        (back_norm_one, 4, 0),
        (back_pick, 2, 0),
        (back_leave, 7, 0),
    ):
        pieces.extend([None] * pause)
        pieces.extend(functools.partial(work, i) for i in range(number))

    def step(t, carry):
        for name, stage in stages:
            n = t - offsets[name]
            pl.when((n >= 0) & (n < count))(functools.partial(stage, n))
        for at, piece in enumerate(pieces):
            if piece is not None:
                pl.when(t == at)(piece)
        return carry

    lax.fori_loop(0, count + offsets["done"], step, 0)
    for n in range(count - SEMS, n_real):
        t_copy(n).wait()
    for k in range(2):
        own_copy(k).wait()
        for d in range(1, 8):
            far(k, d).wait()
    for b in range(BATCHES):
        u_own(b).wait()
        for d in range(1, 8):
            u_back(b, d).wait()


def reduced(inverse, lefts, d_gu, act, smalls, masks, mixer, owned, leaving, scale):
    edges = [0]
    for columns in (3 * D, D, d_gu.shape[1], act.shape[1]):
        edges.append(edges[-1] + columns // COLS)
    rows = act.shape[0]
    count = edges[-1]
    bf16, f32 = jnp.bfloat16, jnp.float32
    anywhere = pl.BlockSpec(memory_space=pl.ANY)
    vmem = pl.BlockSpec(memory_space=pltpu.VMEM)
    return pl.pallas_call(
        functools.partial(reduce_kernel, tuple(edges), scale),
        out_shape=(
            jax.ShapeDtypeStruct((256, (count + 1) * COLS), bf16),
            jax.ShapeDtypeStruct((2, 2, count * 2, 16, BLK), bf16),
            jax.ShapeDtypeStruct((8, count // 2, 16, BLK), bf16),
            jax.ShapeDtypeStruct(leaving.shape, bf16),
            jax.ShapeDtypeStruct(leaving.shape, bf16),
        ),
        in_specs=[
            pl.BlockSpec(memory_space=pltpu.SMEM),
            vmem,
            anywhere,
            anywhere,
            vmem,
            vmem,
        ]
        + [anywhere] * 9,
        out_specs=(anywhere,) * 5,
        scratch_shapes=[
            pltpu.VMEM((SEMS, rows, COLS), bf16),
            pltpu.VMEM((RING, 2, 2, 256, COLS), bf16),
            pltpu.VMEM((RING, 2, 256, COLS), bf16),
            pltpu.VMEM((SEMS, 256, COLS), bf16),
            pltpu.VMEM((RING, 256, COLS), bf16),
            pltpu.VMEM((SEMS, 128, COLS), bf16),
            pltpu.VMEM((RING, 128, COLS), bf16),
            pltpu.VMEM((SEMS, 64, COLS), bf16),
            pltpu.VMEM((RING, 64, COLS), bf16),
            pltpu.VMEM((SEMS, 32, COLS), bf16),
            pltpu.VMEM((RING, 32, COLS), bf16),
            pltpu.VMEM((RING, 256, COLS), bf16),
            pltpu.VMEM((SEMS, 2, 8, 16, BLK), bf16),
            pltpu.VMEM((SEMS, 2, 2, 2, 16, BLK), bf16),
            pltpu.VMEM((8, count // 2, 16, BLK), bf16),
            pltpu.SemaphoreType.DMA((SEMS,)),
            pltpu.SemaphoreType.DMA((SEMS, 2)),
            pltpu.SemaphoreType.DMA((SEMS,)),
            pltpu.SemaphoreType.DMA((SEMS,)),
            pltpu.SemaphoreType.DMA((8, SEMS)),
            pltpu.SemaphoreType.DMA((8, SEMS)),
            pltpu.SemaphoreType.DMA((2, 7)),
            pltpu.SemaphoreType.DMA((2, 7)),
            pltpu.SemaphoreType.DMA((2 + BATCHES,)),
            pltpu.SemaphoreType.DMA((BATCHES, 7)),
            pltpu.SemaphoreType.DMA((BATCHES, 7)),
            pltpu.VMEM(leaving.shape, bf16),
            pltpu.VMEM((rows, D), bf16),
            pltpu.VMEM((rows, 3 * D), f32),
            pltpu.VMEM((rows + 8, D), f32),
            pltpu.VMEM((rows, D), f32),
            pltpu.VMEM((rows, D), f32),
            pltpu.VMEM((8, D, HEAD), bf16),
            pltpu.VMEM((rows + 8, D), f32),
            pltpu.VMEM((rows, 3 * D), bf16),
            pltpu.VMEM((rows, D), bf16),
            pltpu.VMEM(leaving.shape, bf16),
            pltpu.VMEM((BLK, D), f32),
            pltpu.SemaphoreType.DMA((7,)),
            pltpu.SemaphoreType.DMA((2,)),
        ],
        compiler_params=pltpu.CompilerParams(
            collective_id=0, has_side_effects=True, vmem_limit_bytes=62 << 20
        ),
        cost_estimate=pl.CostEstimate(
            flops=2 * rows * 1024 * count * COLS, bytes_accessed=10**9, transcendentals=0
        ),
        name="reduce_chunks",
    )(inverse, lefts, d_gu, act, smalls, masks, *mixer, owned, leaving)


HEAD = 512
TRIO = 256


def forward_kernel(
    deal_ref,
    inverse_ref,
    tokens_ref,
    dy_ref,
    weights_ref,
    small_ref,
    masks_ref,
    roots_ref,
    lefts_ref,
    x_ref,
    dy_out_ref,
    proj_ref,
    prev_ref,
    h_ref,
    act_ref,
    d_gu_ref,
    d_hn_ref,
    result_ref,
    heads_ref,
    smalls_ref,
    owned_ref,
    x_in,
    dy_in,
    heads,
    trios,
    smalls,
    xs,
    dys,
    xn,
    yc,
    hn,
    turned,
    proj,
    mixed,
    total,
    back,
    act_buf,
    d_gu_buf,
    own_sem,
    load_sem,
    far_send,
    far_recv,
    small_send,
    small_recv,
    send_sem,
    recv_sem,
    halo_sem,
    out_sem,
    act_sem,
):
    z, x, y, c = place()
    seq, wsh = lax.axis_index("seq"), lax.axis_index("wsh")
    bf16 = jnp.bfloat16
    n_heads, n_trios = heads.shape[0], trios.shape[0]
    count = n_heads + n_trios
    core_id = (seq, y * 2 + (1 - c))
    y_id = (seq, (1 - y) * 2 + c)
    cross_id = (seq, (1 - y) * 2 + (1 - c))
    x_id = (z * 2 + (1 - x), wsh)
    z_id = ((z + 1 - 2 * (z % 2)) * 2 + x, wsh)
    far_ids = [(lax.rem(seq + d, 8), wsh) for d in range(1, 8)]
    quarter = x * 2 + z % 2
    mine = pl.multiple_of(wsh * 256, 256)
    theirs = pl.multiple_of(((1 - y) * 2 + c) * 256, 256)

    barrier = pltpu.get_barrier_semaphore()
    for device in [core_id, y_id, cross_id] + far_ids:
        pl.semaphore_signal(barrier, inc=1, device_id=device, device_id_type=MESH)
    pl.semaphore_wait(barrier, 10)

    def far(k, d, source, target):
        to = lax.rem(seq + d, 8)
        return pltpu.make_async_remote_copy(
            src_ref=source.at[to],
            dst_ref=target.at[seq],
            send_sem=far_send.at[k, d - 1],
            recv_sem=far_recv.at[k, d - 1],
            device_id=(to, wsh),
            device_id_type=MESH,
        )

    def small_copy(k, to):
        return pltpu.make_async_remote_copy(
            src_ref=small_ref,
            dst_ref=smalls.at[:, pl.ds(mine, 256)],
            send_sem=small_send.at[k],
            recv_sem=small_recv.at[k],
            device_id=to,
            device_id_type=MESH,
        )

    small_ids = (core_id, y_id, cross_id)
    own_copies = (
        pltpu.make_async_copy(tokens_ref.at[seq], x_in.at[seq], own_sem.at[0]),
        pltpu.make_async_copy(dy_ref.at[seq], dy_in.at[seq], own_sem.at[1]),
        pltpu.make_async_copy(small_ref, smalls.at[:, pl.ds(mine, 256)], own_sem.at[2]),
        pltpu.make_async_copy(roots_ref.at[seq], owned_ref.at[seq], own_sem.at[3]),
    )
    for copy in own_copies:
        copy.start()
    for d in range(1, 8):
        far(0, d, tokens_ref, x_in).start()
    for k, to in enumerate(small_ids):
        small_copy(k, to).start()

    def head_loads(u):
        at = u * HEAD if isinstance(u, int) else pl.multiple_of(u * HEAD, HEAD)
        return [
            pltpu.make_async_copy(
                weights_ref.at[:, pl.ds(at, HEAD)],
                heads.at[u, pl.ds(mine, 256)],
                load_sem.at[u],
            )
        ]

    def trio_loads(k, sem):
        first = n_heads * HEAD
        return [
            pltpu.make_async_copy(
                weights_ref.at[
                    :,
                    pl.ds(
                        pl.multiple_of(first + part * n_trios * TRIO + k * TRIO, TRIO), TRIO
                    ),
                ],
                trios.at[k, pl.ds(mine, 256), pl.ds(part * TRIO, TRIO)],
                load_sem.at[n_heads + part * n_trios + k],
            )
            for part in range(3)
        ]

    def remote(flow, buf, i, unit, first, rows, to):
        piece = buf.at[i, pl.ds(pl.multiple_of(first, 16), rows)]
        return pltpu.make_async_remote_copy(
            src_ref=piece,
            dst_ref=piece,
            send_sem=send_sem.at[flow, unit],
            recv_sem=recv_sem.at[flow, unit],
            device_id=to,
            device_id_type=MESH,
        )

    def copies(buf, i, unit):
        near = mine + quarter * 64
        wide = mine + (3 - quarter) * 64
        got = theirs + quarter * 64
        other = mine + (quarter + 1 - 2 * (z % 2)) * 64 + 48
        table = {
            "core": (0, mine, 256, core_id),
            "near": (1, near, 64, y_id),
            "wide": (2, wide, 64, y_id),
            "x": (3, got, 64, x_id),
            "z": (4, got, 48, z_id),
            "rest": (6, other, 16, y_id),
            "pass": (5, theirs, 256, core_id),
        }

        def pick(name):
            flow, first, rows, to = table[name]
            return remote(flow, buf, i, unit, first, rows, to)

        return pick

    def head(u):
        return copies(heads, u, u)

    def trio(k):
        return copies(trios, k, n_heads + k)

    def send_first(c3):
        c3("near").start()
        c3("wide").start()
        c3("rest").start()
        c3("core").start()

    def send_on(c3):
        c3("near").wait()
        c3("x").start()
        c3("z").start()

    def hand_over(c3):
        c3("wide").wait()
        c3("rest").wait()
        c3("x").wait()
        c3("z").wait()
        c3("pass").start()

    def arrived(c3):
        c3("core").wait()
        c3("pass").wait()

    for u in range(n_heads):
        for copy in head_loads(u):
            copy.start()

    def load_trio(k, carry):
        for copy in trio_loads(k, None):
            copy.start()
        return carry

    lax.fori_loop(0, n_trios, load_trio, 0)
    for u in range(n_heads):
        for copy in head_loads(u):
            copy.wait()
        send_first(head(u))

    def first_trio(k, carry):
        for copy in trio_loads(k, None):
            copy.wait()
        send_first(trio(k))
        return carry

    lax.fori_loop(0, n_trios, first_trio, 0)
    send_on(head(0))
    send_on(head(1))

    def turn(source, r, wait):
        copy = pltpu.make_async_copy(turned, lefts_ref.at[r], out_sem.at[0])
        if wait:
            copy.wait()
        for j in range(8):
            turned[j * 128 : (j + 1) * 128, :] = source[:, j * 128 : (j + 1) * 128].T
        copy.start()

    for d in range(1, 8):
        far(0, d, tokens_ref, x_in).wait()
    own_copies[0].wait()
    for k, to in enumerate(small_ids):
        small_copy(k, to).wait()
    own_copies[2].wait()
    gain_one = smalls[0:1, :].astype(jnp.float32)
    for k in range(8):
        rows = slice(k * 64, (k + 1) * 64)
        unit = x_in[deal_ref[k]]
        xs[rows] = unit
        value = unit.astype(jnp.float32)
        xn[rows] = (value * rms_scale(value) * gain_one).astype(bf16)
    turn(xn, 0, False)

    def mixer_unit(u):
        proj[:, u * HEAD : (u + 1) * HEAD] = jnp.dot(
            xn[...], heads[u], preferred_element_type=jnp.float32
        )

    for u in range(n_heads + 2):
        if 2 <= u < n_heads:
            send_on(head(u))
        if u < 7:
            far(1, u + 1, dy_ref, dy_in).start()
        if u >= 1 and u - 1 < n_heads:
            hand_over(head(u - 1))
        if u >= 2:
            arrived(head(u - 2))
            if u - 2 < 6:
                mixer_unit(u - 2)

    out_proj = pltpu.make_async_copy(proj, proj_ref, out_sem.at[1])
    out_proj.start()
    width = D
    halo = slice(0, 8)
    for i in range(4):
        rows = slice(i * 128, (i + 1) * 128)
        back[8 + i * 128 : 8 + (i + 1) * 128] = proj[rows, :width] * proj[rows, 2 * width :]
    ring = pltpu.make_async_remote_copy(
        src_ref=back.at[pl.ds(512, 8)],
        dst_ref=mixed,
        send_sem=halo_sem.at[0],
        recv_sem=halo_sem.at[1],
        device_id=far_ids[0],
        device_id_type=MESH,
    )
    ring.start()
    send_on(trio(0))
    for d in range(1, 8):
        far(1, d, dy_ref, dy_in).wait()
    own_copies[1].wait()
    for k in range(8):
        dys[k * 64 : (k + 1) * 64] = dy_in[deal_ref[k]]
    turn(dys, 3, True)
    ring.wait()
    back[halo] = mixed[...]
    taps = [smalls[2 + k : 3 + k, :].astype(jnp.float32) for k in range(3)]
    for i in range(8):
        first = i * 64
        rows = slice(first, first + 64)
        conv = (
            taps[0] * masks_ref[0, rows] * back[first + 6 : first + 70]
            + taps[1] * masks_ref[1, rows] * back[first + 7 : first + 71]
            + taps[2] * back[first + 8 : first + 72]
        )
        yc[rows] = (proj[rows, width : 2 * width] * conv).astype(bf16)
    hand_over(trio(0))
    for u in range(6, n_heads):
        lanes = slice((u - 6) * HEAD, (u - 5) * HEAD)
        total[:, lanes] = xs[:, lanes].astype(jnp.float32) + jnp.dot(
            yc[...], heads[u], preferred_element_type=jnp.float32
        )
    out_h = pltpu.make_async_copy(total, h_ref, out_sem.at[2])
    out_h.start()
    gain_two = smalls[1:2, :].astype(jnp.float32)
    for i in range(8):
        rows = slice(i * 64, (i + 1) * 64)
        value = total[rows]
        hn[rows] = (value * rms_scale(value) * gain_two).astype(bf16)
    for i in range(4):
        back[i * 128 : (i + 1) * 128] = jnp.zeros((128, width), jnp.float32)
    send_on(trio(1))
    turn(yc, 1, True)
    out_h.wait()

    def act_copies(k, slot):
        at = pl.multiple_of(k * TRIO, TRIO)
        up = pl.multiple_of((n_trios + k) * TRIO, TRIO)
        return (
            pltpu.make_async_copy(
                act_buf.at[slot], act_ref.at[:, pl.ds(at, TRIO)], act_sem.at[slot, 0]
            ),
            pltpu.make_async_copy(
                d_gu_buf.at[slot, :, pl.ds(0, TRIO)],
                d_gu_ref.at[:, pl.ds(at, TRIO)],
                act_sem.at[slot, 1],
            ),
            pltpu.make_async_copy(
                d_gu_buf.at[slot, :, pl.ds(TRIO, TRIO)],
                d_gu_ref.at[:, pl.ds(up, TRIO)],
                act_sem.at[slot, 2],
            ),
        )

    def ffn(k, carry):
        pl.when(k + 2 < n_trios)(lambda: send_on(trio(k + 2)))
        pl.when(k + 1 < n_trios)(lambda: hand_over(trio(k + 1)))
        arrived(trio(k))
        pl.when(k < 7)(lambda: far(2, k + 1, roots_ref, owned_ref).start())
        slot = lax.rem(k, 2)

        @pl.when(k >= 2)
        def _():
            for copy in act_copies(k - 2, slot):
                copy.wait()

        gate = jnp.dot(hn[...], trios[k, :, :TRIO], preferred_element_type=jnp.float32)
        upper = jnp.dot(
            hn[...], trios[k, :, TRIO : 2 * TRIO], preferred_element_type=jnp.float32
        )
        d_act = jnp.dot(dys[...], trios[k, :, 2 * TRIO :], preferred_element_type=jnp.float32)
        sig = jax.nn.sigmoid(gate)
        silu = gate * sig
        act_buf[slot] = (silu * upper).astype(bf16)
        d_gu_buf[slot, :, :TRIO] = (
            d_act * upper * sig * (1.0 + gate * (1.0 - sig))
        ).astype(bf16)
        d_gu_buf[slot, :, TRIO:] = (d_act * silu).astype(bf16)
        for copy in act_copies(k, slot):
            copy.start()
        total[...] += contract_cols(act_buf[slot], trios[k, :, 2 * TRIO :])
        back[0:512] += contract_cols(d_gu_buf[slot], trios[k, :, : 2 * TRIO])
        return carry

    lax.fori_loop(0, n_trios, ffn, 0)
    turn(hn, 2, True)
    out_back = pltpu.make_async_copy(back.at[pl.ds(0, 512)], d_hn_ref, out_sem.at[3])
    out_back.start()
    for k in range(8):
        x_in[k] = total[k * 64 : (k + 1) * 64].astype(bf16)
    for k in range(8):
        dy_in[k] = x_in[inverse_ref[k]]
    last = (
        pltpu.make_async_copy(dy_in, result_ref, out_sem.at[4]),
        pltpu.make_async_copy(xs, x_ref, out_sem.at[5]),
        pltpu.make_async_copy(dys, dy_out_ref, out_sem.at[6]),
        pltpu.make_async_copy(smalls, smalls_ref, out_sem.at[7]),
        pltpu.make_async_copy(mixed, prev_ref, out_sem.at[8]),
        pltpu.make_async_copy(heads, heads_ref, out_sem.at[9]),
    )
    for copy in last:
        copy.start()
    for k in range(n_trios - 2, n_trios):
        for copy in act_copies(k, k % 2):
            copy.wait()
    for copy in last:
        copy.wait()
    for d in range(1, 8):
        far(2, d, roots_ref, owned_ref).wait()
    own_copies[3].wait()
    out_proj.wait()
    out_back.wait()
    pltpu.make_async_copy(turned, lefts_ref.at[2], out_sem.at[0]).wait()


def gathered_forward(deal_order, inverse, tokens, dys, weights, small, masks, roots):
    bf16, f32 = jnp.bfloat16, jnp.float32
    rows = tokens.shape[0] * tokens.shape[1]
    n_heads = 4 * D // HEAD
    n_trios = FF // TRIO
    count = n_heads + n_trios
    anywhere = pl.BlockSpec(memory_space=pl.ANY)
    vmem = pl.BlockSpec(memory_space=pltpu.VMEM)
    shape = jax.ShapeDtypeStruct
    return pl.pallas_call(
        forward_kernel,
        out_shape=(
            shape((4, D, rows), bf16),
            shape((rows, D), bf16),
            shape((rows, D), bf16),
            shape((rows, 3 * D), f32),
            shape((8, D), f32),
            shape((rows, D), f32),
            shape((rows, FF), bf16),
            shape((rows, 2 * FF), bf16),
            shape((rows, D), f32),
            shape(tokens.shape, bf16),
            shape((n_heads, D, HEAD), bf16),
            shape((8, D), bf16),
            shape(roots.shape, bf16),
        ),
        in_specs=[
            pl.BlockSpec(memory_space=pltpu.SMEM),
            pl.BlockSpec(memory_space=pltpu.SMEM),
            anywhere,
            anywhere,
            anywhere,
            vmem,
            vmem,
            anywhere,
        ],
        out_specs=(anywhere,) * 13,
        scratch_shapes=[
            pltpu.VMEM(tokens.shape, bf16),
            pltpu.VMEM(tokens.shape, bf16),
            pltpu.VMEM((n_heads, D, HEAD), bf16),
            pltpu.VMEM((n_trios, D, 3 * TRIO), bf16),
            pltpu.VMEM((8, D), bf16),
            pltpu.VMEM((rows, D), bf16),
            pltpu.VMEM((rows, D), bf16),
            pltpu.VMEM((rows, D), bf16),
            pltpu.VMEM((rows, D), bf16),
            pltpu.VMEM((rows, D), bf16),
            pltpu.VMEM((D, rows), bf16),
            pltpu.VMEM((rows, 3 * D), f32),
            pltpu.VMEM((8, D), f32),
            pltpu.VMEM((rows, D), f32),
            pltpu.VMEM((rows + 8, D), f32),
            pltpu.VMEM((2, rows, TRIO), bf16),
            pltpu.VMEM((2, rows, 2 * TRIO), bf16),
            pltpu.SemaphoreType.DMA((4,)),
            pltpu.SemaphoreType.DMA((n_heads + 3 * n_trios,)),
            pltpu.SemaphoreType.DMA((3, 7)),
            pltpu.SemaphoreType.DMA((3, 7)),
            pltpu.SemaphoreType.DMA((3,)),
            pltpu.SemaphoreType.DMA((3,)),
            pltpu.SemaphoreType.DMA((7, count)),
            pltpu.SemaphoreType.DMA((7, count)),
            pltpu.SemaphoreType.DMA((2,)),
            pltpu.SemaphoreType.DMA((10,)),
            pltpu.SemaphoreType.DMA((2, 3)),
        ],
        compiler_params=pltpu.CompilerParams(
            collective_id=1, has_side_effects=True, vmem_limit_bytes=63 << 20
        ),
        cost_estimate=pl.CostEstimate(
            flops=8 * rows * D * FF, bytes_accessed=10**8, transcendentals=0
        ),
        name="gathered_forward",
    )(deal_order, inverse, tokens, dys, weights, small, masks, roots)


PARTS = 7


def closing_kernel(
    grad_in, vec_in, terms_in, stats_in, update_in, state_in, grad, vec, state, step, stats, update
):
    grad[...] = grad_in[...].astype(jnp.float32)
    stats[...] = BETA * stats_in[...] + ((1.0 - BETA) / BLK) * terms_in[...].astype(jnp.float32)
    for i in range(update_in.shape[0]):
        for m in range(update_in.shape[1]):
            update[i, :, m] = -LEARN * update_in[i, m].astype(jnp.float32)

    @pl.when(pl.program_id(0) == 0)
    def _():
        count = vec.shape[0]
        turned = vec_in[:, :BLK].astype(jnp.float32).T[:count]
        fresh = BETA_VEC * state_in[...] + (1.0 - BETA_VEC) * turned * turned
        vec[...] = turned
        state[...] = fresh
        step[...] = -LEARN_VEC * turned * lax.rsqrt(fresh)


def closing(grad_bf, terms, kron_stats, update, vector_state):
    f32 = jnp.float32
    rows, wide = grad_bf.shape
    columns = wide - COLS
    kinds, blocks, share, _ = kron_stats.shape
    nrow, ncol = rows // BLK, columns // BLK
    shape = jax.ShapeDtypeStruct
    vec_spec = pl.BlockSpec(vector_state.shape, lambda g: (0, 0))
    grad_spec = pl.BlockSpec((rows, columns // PARTS), lambda g: (0, g))
    stat_spec = pl.BlockSpec((kinds, blocks // PARTS, share, BLK), lambda g: (0, g, 0, 0))
    groups = ncol // 4
    outs = pl.pallas_call(
        closing_kernel,
        grid=(PARTS,),
        out_shape=(
            shape((rows, columns), f32),
            shape(vector_state.shape, f32),
            shape(vector_state.shape, f32),
            shape(vector_state.shape, f32),
            shape(kron_stats.shape, f32),
            shape((nrow, groups, 4, share, BLK), f32),
        ),
        in_specs=[
            grad_spec,
            pl.BlockSpec((rows, COLS), lambda g: (0, columns // COLS)),
            stat_spec,
            stat_spec,
            pl.BlockSpec((nrow, 4, groups // PARTS, share, BLK), lambda g: (0, 0, g, 0, 0)),
            vec_spec,
        ],
        out_specs=(
            grad_spec,
            vec_spec,
            vec_spec,
            vec_spec,
            stat_spec,
            pl.BlockSpec((nrow, groups // PARTS, 4, share, BLK), lambda g: (0, g, 0, 0, 0)),
        ),
        compiler_params=pltpu.CompilerParams(vmem_limit_bytes=40 << 20),
        name="closing",
    )(
        grad_bf,
        grad_bf,
        terms.reshape(kron_stats.shape),
        kron_stats,
        update.reshape(nrow, 4, groups, share, BLK),
        vector_state,
    )
    return (*outs[:5], outs[5].reshape(blocks, share, BLK))


def shards(
    tokens_in,
    out_grad,
    deal_order,
    seq_lengths,
    weights,
    norm_gains,
    conv_kernel,
    vector_state,
    kron_stats,
    kron_roots,
):
    n_seq = lax.axis_size("seq")
    n_wsh = lax.axis_size("wsh")
    rows = tokens_in.shape[1]
    unit = rows // n_seq
    first_row = lax.axis_index("seq") * rows
    pos = seq_positions(seq_lengths[0], first_row, rows + 8)
    masks = jnp.stack([(pos >= 2 - k).astype(jnp.float32)[:, None] for k in range(2)])
    classes = jnp.arange(n_seq, dtype=jnp.int32)
    inverse = jnp.sum(
        jnp.where(deal_order[None, :] == classes[:, None], classes[None, :], 0), axis=1
    )
    nrow_blocks, ncol_blocks = weights.shape[0] // BLK, weights.shape[1] // BLK
    share = BLK // n_seq
    roots = kron_roots.astype(jnp.bfloat16).reshape(
        2, nrow_blocks, ncol_blocks // 4, 4, share, BLK
    )
    roots = roots.transpose(1, 3, 0, 2, 4, 5).reshape(n_seq, 2, ncol_blocks // 4, share, BLK)
    small = jnp.concatenate(
        [norm_gains, conv_kernel, jnp.zeros((3, norm_gains.shape[1]), jnp.bfloat16)], axis=0
    )
    (
        lefts,
        x_bf,
        dy_bf,
        proj,
        prev,
        hidden_sum,
        act,
        d_gu,
        d_hn,
        result,
        heads,
        smalls,
        owned,
    ) = gathered_forward(
        deal_order,
        inverse,
        tokens_in.reshape(n_seq, unit, D),
        out_grad.reshape(n_seq, unit, D),
        weights,
        small,
        masks,
        roots,
    )
    grad_bf, terms, update, out_back, dx_back = reduced(
        inverse,
        lefts,
        d_gu,
        act,
        smalls,
        masks,
        (x_bf.reshape(n_seq, unit, D), dy_bf, proj, prev, hidden_sum, d_hn, heads),
        owned,
        result,
        float((rows * n_seq * n_wsh) ** -0.5),
    )
    grad_shard, vec_grad, state_new, vec_update, stats_new, update = closing(
        grad_bf, terms, kron_stats, update, vector_state
    )
    return (
        out_back.reshape(1, rows, D),
        dx_back.reshape(1, rows, D),
        grad_shard,
        vec_grad,
        state_new,
        vec_update,
        stats_new,
        update,
    )


def solution(mesh):
    known = mesh.shape["seq"] == 8 and mesh.shape["wsh"] == 4
    return jax.shard_map(
        shards if known else plain_shards,
        mesh=mesh,
        in_specs=(
            P("wsh", "seq", None),
            P("wsh", "seq", None),
            P(),
            P("wsh", None),
            P("wsh", None),
            P(None, "wsh"),
            P(None, "wsh"),
            P(None, "wsh"),
            P(None, "wsh", "seq", None),
            P(None, "wsh", "seq", None),
        ),
        out_specs=(
            P("wsh", "seq", None),
            P("wsh", "seq", None),
            P("wsh", None),
            P(None, "wsh"),
            P(None, "wsh"),
            P(None, "wsh"),
            P(None, "wsh", "seq", None),
            P("wsh", "seq", None),
        ),
        check_vma=False,
    )
```
